32 devices in a mesh: dom: 32 (over z, y, x, core).
Axes of the slice: x: 2, y: 2, z: 4, core: 2. Of those that a mesh axis runs over, the one named last changes fastest.
Arguments:
- features: bfloat16 [131072, 256], P('dom'), may hold values from -6 to 6
- weight: bfloat16 [256, 256], replicated, may hold values from -0.375 to 0.375
- bias_vector: float32 [256], replicated, may hold values from -3 to 3
- tile_values: bfloat16 [8192, 128, 128], P('dom'), may hold values from -0.1875 to 0.1875
- tile_row: int32 [32, 256], P('dom'), may hold values from 0 to 31
- tile_col: int32 [32, 256], P('dom'), may hold values from 0 to 35
- tile_count: int32 [32], P('dom'), may hold values from 64 to 256, as said below
- send_rows: int32 [32, 32, 16], P('dom'), may hold values from 0 to 4095, as said below
- send_count: int32 [32, 32], P('dom'), may hold values from 0 to 16, as said below
- cotangent: bfloat16 [131072, 256], P('dom'), may hold values from -6 to 6
Outputs:
- activation: bfloat16 [131072, 256], P('dom')
- grad_features: bfloat16 [131072, 256], P('dom')
- grad_weight: float32 [256, 256], replicated
- grad_bias: float32 [256], replicated
The draws below stay inside these ranges and needn't reach their ends.
Inputs may be any that keep to these rules, and one draw needn't show every extreme that they name: `tile_count`: each partition uses at least a quarter of its slots; in every draw two partitions use all 256. `send_rows`: for each sender and reader the 16 listed rows are distinct. `send_count`: in every draw one reader receives 16 rows from every partition.
All inputs are finite; a program needn't handle non-finite values.
Results may differ from the reference program's by a relative error of at most 0.0061.
Values may be sent and summed in bfloat16 or wider, within the bound.
A program may use at most 192 MiB of HBM per device.

```python
import jax
import jax.numpy as jnp
from jax import lax

F = 256
TB = 128
TPB = 8
SLOT = 16
ROWS_DEV = 4096
NB = 32
KMAX = 256
EB = 36
NODES = 131072
N_DOM = 32


def draw_tile_count(key, part):
    first_key, second_key = jax.random.split(jax.random.fold_in(key, 5))
    base_counts = jax.random.randint(first_key, (N_DOM,), KMAX // 4, KMAX // 2 + 1)
    shuffled = jax.random.permutation(second_key, N_DOM)
    return jnp.where(shuffled < 2, KMAX, base_counts).astype(jnp.int32)


def draw_send_rows(key, part):
    first_key, second_key = jax.random.split(jax.random.fold_in(key, 11))
    beginning = jax.random.randint(first_key, (N_DOM, N_DOM, 1), 0, ROWS_DEV)
    increments = jax.random.randint(second_key, (N_DOM, N_DOM, SLOT), 1, ROWS_DEV // SLOT + 1)
    increments = increments.at[:, :, 0].set(0)
    return ((beginning + jnp.cumsum(increments, axis=2)) % ROWS_DEV).astype(jnp.int32)


def draw_send_count(key, part):
    first_key, second_key = jax.random.split(jax.random.fold_in(key, 23))
    counts_drawn = jax.random.randint(first_key, (N_DOM, N_DOM), 0, SLOT + 1)
    full_reader = jax.random.randint(second_key, (), 0, N_DOM)
    column_ids = lax.broadcasted_iota(jnp.int32, (N_DOM, N_DOM), 1)
    return jnp.where(column_ids == full_reader, SLOT, counts_drawn).astype(jnp.int32)


def touch_ends(values, own_key, smallest, high):
    spot = [jax.random.randint(jax.random.fold_in(own_key, axis), (), 0, length) for axis, length in enumerate(values.shape)]
    longest = values.shape.index(max(values.shape))
    beside = spot[:longest] + [(spot[longest] + 1) % values.shape[longest]] + spot[longest + 1:]
    return values.at[tuple(spot)].set(smallest).at[tuple(beside)].set(high)


def shard_levels(key, dims, pieces, low, largest):
    level = 1.0
    for dim, blocks in pieces:
        steps = jax.random.uniform(jax.random.fold_in(jax.random.fold_in(key, 6), dim), (blocks,), jnp.float32, low / len(pieces), largest / len(pieces))
        level = level * jnp.repeat(jnp.exp(steps), dims[dim] // blocks).reshape((-1,) + (1,) * (len(dims) - 1 - dim))
    return level


def gaussian(stream_key, dims, deviation, bound, cuts=(), kind=jnp.bfloat16):
    values = jax.random.normal(stream_key, dims, jnp.float32) * deviation
    if len(cuts) > 0:
        values = shard_levels(stream_key, dims, cuts, -0.22, 0.18) * values
    return jnp.clip(values, min=-bound, max=bound).astype(kind)


def setup_inputs(seed: int = 0) -> dict:
    keys = jax.random.split(jax.random.key(seed), 11)
    features = gaussian(keys[0], (NODES, F), 1.0, 6.0, ((0, 32),))
    weight = gaussian(keys[1], (F, F), F ** -0.5, 0.375)
    bias_vector = gaussian(keys[2], (F,), 0.5, 3.0, (), jnp.float32)
    tile_values = gaussian(keys[3], (N_DOM * KMAX, TB, TB), (TB * TPB) ** -0.5, 0.1875, ((0, 32),))
    tile_row = touch_ends(jax.random.randint(keys[4], (N_DOM, KMAX), 0, NB), jax.random.fold_in(keys[4], 1), 0, NB - 1).astype(jnp.int32)
    tile_col = touch_ends(jax.random.randint(keys[5], (N_DOM, KMAX), 0, EB), jax.random.fold_in(keys[5], 1), 0, EB - 1).astype(jnp.int32)
    tile_count = draw_tile_count(jax.random.fold_in(keys[10], 71), 0)
    send_rows = draw_send_rows(jax.random.fold_in(keys[10], 71), 0)
    send_count = draw_send_count(jax.random.fold_in(keys[10], 71), 0)
    cotangent = gaussian(keys[9], (NODES, F), 1.0, 6.0, ((0, 32),))
    return dict(features=features, weight=weight, bias_vector=bias_vector, tile_values=tile_values, tile_row=tile_row, tile_col=tile_col, tile_count=tile_count, send_rows=send_rows, send_count=send_count, cotangent=cotangent)


def reference(features, weight, bias_vector, tile_values, tile_row, tile_col, tile_count, send_rows, send_count, cotangent):
    feature_width = features.shape[1]
    feature_parts = features.reshape(N_DOM, ROWS_DEV, feature_width)
    tile_parts = tile_values.reshape(N_DOM, KMAX, TB, TB)
    slot_index = jnp.arange(SLOT, dtype=jnp.int32)
    live_slots = slot_index[None, None, :] < send_count[:, :, None]
    device_ids = jnp.arange(N_DOM, dtype=jnp.int32)
    tile_ids = jnp.arange(KMAX, dtype=jnp.int32)

    def outgoing(owner_index):
        picked = feature_parts[owner_index][send_rows[owner_index]]
        return jnp.where(live_slots[owner_index][:, :, None], picked, jnp.zeros_like(picked))

    outbound = lax.map(outgoing, device_ids)
    halo_rows = jnp.swapaxes(outbound, 0, 1)

    def forward(reader_index):
        extended = jnp.concatenate([feature_parts[reader_index], halo_rows[reader_index].reshape(N_DOM * SLOT, feature_width)], 0)
        ext_blocks = extended.reshape(EB, TB, feature_width)
        fetched = ext_blocks[tile_col[reader_index]].astype(jnp.float32)
        products = jnp.einsum("kij,kjf->kif", tile_parts[reader_index].astype(jnp.float32), fetched, precision=lax.Precision.HIGHEST)
        selected = tile_ids < tile_count[reader_index]
        levels = jnp.arange(NB, dtype=jnp.int32)
        one_hot = ((tile_row[reader_index][None, :] == levels[:, None]) & selected[None, :]).astype(jnp.float32)
        summed = jnp.dot(one_hot, products.reshape(KMAX, -1), precision=lax.Precision.HIGHEST)
        return summed.reshape(ROWS_DEV, feature_width).astype(jnp.bfloat16)

    aggregated = lax.map(forward, device_ids).reshape(NODES, feature_width)
    linear = jnp.dot(aggregated, weight, preferred_element_type=jnp.float32) + bias_vector
    sigmoid_value = jax.nn.sigmoid(linear)
    activation = (linear * sigmoid_value).astype(jnp.bfloat16)
    slope_value = sigmoid_value * (1.0 + linear * (1.0 - sigmoid_value))
    grad_linear = (cotangent.astype(jnp.float32) * slope_value).astype(jnp.bfloat16)
    norm_scale = NODES ** -0.5
    grad_weight = jnp.dot(aggregated.T, grad_linear, preferred_element_type=jnp.float32) * norm_scale
    grad_bias = jnp.sum(grad_linear.astype(jnp.float32), axis=0) * norm_scale
    grad_mixed = jnp.dot(grad_linear, weight.T, preferred_element_type=jnp.float32).astype(jnp.bfloat16)
    mixed_parts = grad_mixed.reshape(N_DOM, NB, TB, feature_width)

    def backward(reader_index):
        fetched = mixed_parts[reader_index][tile_row[reader_index]].astype(jnp.float32)
        products = jnp.einsum("kji,kjf->kif", tile_parts[reader_index].astype(jnp.float32), fetched, precision=lax.Precision.HIGHEST)
        selected = tile_ids < tile_count[reader_index]
        levels = jnp.arange(EB, dtype=jnp.int32)
        one_hot = ((tile_col[reader_index][None, :] == levels[:, None]) & selected[None, :]).astype(jnp.float32)
        summed = jnp.dot(one_hot, products.reshape(KMAX, -1), precision=lax.Precision.HIGHEST)
        summed = summed.reshape(EB * TB, feature_width)
        own_part = summed[:ROWS_DEV]
        halo_part = summed[ROWS_DEV:].astype(jnp.bfloat16).reshape(N_DOM, SLOT, feature_width)
        return own_part, halo_part

    own_grad, halo_grad = lax.map(backward, device_ids)

    def collect(owner_index):
        incoming = halo_grad[:, owner_index].astype(jnp.float32)
        incoming = jnp.where(live_slots[owner_index][:, :, None], incoming, jnp.zeros_like(incoming))
        return jax.ops.segment_sum(incoming.reshape(-1, feature_width), send_rows[owner_index].reshape(-1), num_segments=ROWS_DEV)

    collected = lax.map(collect, device_ids)
    grad_features = (own_grad + collected).reshape(NODES, feature_width).astype(jnp.bfloat16)
    return (activation, grad_features, grad_weight, grad_bias)
```

```python
import functools
import math

import jax
import jax.numpy as jnp
from jax import lax
from jax.experimental import pallas as pl
from jax.experimental.pallas import tpu as pltpu
from jax.sharding import PartitionSpec as P

MESH = pl.DeviceIdType.MESH
VMEM = pltpu.VMEM
f32 = jnp.float32
bf16 = jnp.bfloat16


def greet(n, me):
    barrier = pltpu.get_barrier_semaphore()

    def signal(i, carry):
        pl.semaphore_signal(
            barrier, inc=1, device_id=(lax.rem(me + i, n),), device_id_type=MESH
        )
        return carry

    lax.fori_loop(1, n, signal, 0)
    return barrier


def push(n, me, src, dst, send_sem, recv_sem, i):
    peer = lax.rem(me + i, n)
    return pltpu.make_async_remote_copy(
        src_ref=src(peer),
        dst_ref=dst.at[me],
        send_sem=send_sem.at[i],
        recv_sem=recv_sem.at[i],
        device_id=(peer,),
        device_id_type=MESH,
    )


def choose(n, count_ref, rows_ref, wide):
    slots, lanes = rows_ref.shape[0], wide.shape[1]
    slot = lax.broadcasted_iota(jnp.int32, (slots, 1), 0)
    for p in range(n):
        column = jnp.where(slot < count_ref[0, p], rows_ref[:, p : p + 1], -1)
        wide[pl.ds(p * slots, slots), :] = jnp.broadcast_to(column, (slots, lanes))


def gather_kernel(
    n, count_ref, rows_ref, features_hbm, halo_ref, chosen_ref,
    features_ref, wide, total, sent, landed, send_sem, recv_sem, load_sem,
):
    me = lax.axis_index("dom")
    slots = wide.shape[0]
    rows = features_ref.shape[0]
    step = math.gcd(rows, 512)
    loads = []
    for c in range(rows // step):
        span = pl.ds(c * step, step)
        loads.append(
            pltpu.make_async_copy(features_hbm.at[span], features_ref.at[span], load_sem.at[c])
        )
        loads[c].start()
    barrier = greet(n, me)
    choose(n, count_ref, rows_ref, wide)
    lane = lax.broadcasted_iota(jnp.int32, wide.shape, 1)
    lanes = wide.shape[1]
    for c in range(rows // step):
        hot = jnp.concatenate(
            [
                jnp.where(wide[...] == lane + (c * step + j), 1.0, 0.0).astype(bf16)
                for j in range(0, step, lanes)
            ],
            axis=1,
        )
        loads[c].wait()
        part = jnp.dot(hot, features_ref[pl.ds(c * step, step), :], preferred_element_type=f32)
        if c == 0:
            total[...] = part
        else:
            total[...] += part
    sent[...] = total[...].astype(bf16).reshape(sent.shape)
    pl.semaphore_wait(barrier, n - 1)
    copy = functools.partial(push, n, me, lambda p: sent.at[p], landed, send_sem, recv_sem)

    def start(i, carry):
        copy(i).start()
        return carry

    def finish(i, carry):
        copy(i).wait()
        return carry

    lax.fori_loop(1, n, start, 0)
    landed[me] = sent[me]
    chosen_ref[...] = wide[...].T[:1, :]
    lax.fori_loop(1, n, finish, 0)
    halo_ref[...] = landed[...]


LANES = 128


def exchange_gather(n, send_count, send_rows, features):
    width = features.shape[1]
    slot_count = send_rows.shape[0]
    slots = n * slot_count
    block = (n, slot_count, width)
    vmem = pl.BlockSpec(memory_space=VMEM)
    return pl.pallas_call(
        functools.partial(gather_kernel, n),
        out_shape=(
            jax.ShapeDtypeStruct(block, bf16),
            jax.ShapeDtypeStruct((1, slots), jnp.int32),
        ),
        in_specs=[
            pl.BlockSpec(memory_space=pltpu.SMEM),
            vmem,
            pl.BlockSpec(memory_space=pltpu.HBM),
        ],
        out_specs=(vmem, vmem),
        scratch_shapes=[
            VMEM(features.shape, bf16),
            VMEM((slots, LANES), jnp.int32),
            VMEM((slots, width), f32),
            VMEM(block, bf16),
            VMEM(block, bf16),
            pltpu.SemaphoreType.DMA((n,)),
            pltpu.SemaphoreType.DMA((n,)),
            pltpu.SemaphoreType.DMA((features.shape[0] // math.gcd(features.shape[0], 512),)),
        ],
        compiler_params=pltpu.CompilerParams(
            collective_id=0, has_side_effects=True, vmem_limit_bytes=60 * 1024 * 1024
        ),
        name="gather_exchange",
    )(send_count, send_rows, features)


GROUP = 8
CHUNK = 16


def local_kernel(
    tile_row, tile_col, tile_count, features, halo, tiles, cotangent, weight, bias,
    activation, own_grad, halo_grad, weight_part, bias_part,
    source, held, cot, act, mixed, forward, backward, spread, wsum, bsum,
    in_sem, tile_sem, cot_sem, act_sem, out_sem,
):
    own = features.shape[0]
    ext = own + halo.shape[0]
    number = tiles.shape[0]
    chunk = math.gcd(number, CHUNK)
    group = math.gcd(chunk, GROUP)
    total = tile_count[0]
    chunks = (total + chunk - 1) // chunk

    def tile_copy(c):
        span = pl.ds(c * chunk, chunk)
        return pltpu.make_async_copy(tiles.at[span], held.at[span], tile_sem.at[c])

    copies = [
        pltpu.make_async_copy(features, source.at[pl.ds(0, own)], in_sem.at[0]),
        pltpu.make_async_copy(halo, source.at[pl.ds(own, ext - own)], in_sem.at[1]),
    ]
    for copy in copies:
        copy.start()

    @pl.loop(0, chunks)
    def _(c):
        tile_copy(c).start()

    cot_copy = pltpu.make_async_copy(cotangent, cot, cot_sem)
    cot_copy.start()

    @pl.loop(0, own)
    def _(r):
        forward[r] = jnp.zeros(forward.shape[1:], f32)
        backward[r] = jnp.zeros(backward.shape[1:], f32)

    for r in range(own, ext):
        backward[r] = jnp.zeros(backward.shape[1:], f32)
    for copy in copies:
        copy.wait()

    @pl.loop(0, chunks)
    def _(c):
        tile_copy(c).wait()
        for g in range(chunk // group):
            base = c * chunk + g * group
            for j in range(group):
                k = base + j
                product = jnp.dot(held[k], source[tile_col[0, k]], preferred_element_type=f32)
                target = jnp.where(k < total, tile_row[0, k], own)
                forward[target] += product

    cot_copy.wait()
    edge = tiles.shape[1]
    step = math.gcd(own, 4)
    width = weight.shape[0]
    wsum[...] = jnp.zeros_like(wsum)
    bsum[...] = jnp.zeros_like(bsum)

    def act_copy(b):
        span = pl.ds(b * step, step)
        return pltpu.make_async_copy(act.at[span], activation.at[span], act_sem.at[b])

    @pl.loop(0, own // step)
    def _(b):
        span = pl.ds(b * step, step)
        agg = forward[span].astype(bf16).reshape(step * edge, width)
        linear = jnp.dot(agg, weight[...], preferred_element_type=f32) + bias[...]
        sig = jax.nn.sigmoid(linear)
        act[span] = (linear * sig).astype(bf16).reshape(step, edge, width)
        act_copy(b).start()
        slope = sig * (1.0 + linear * (1.0 - sig))
        grad = (cot[span].reshape(step * edge, width).astype(f32) * slope).astype(bf16)
        wsum[...] += lax.dot_general(
            agg, grad, (((0,), (0,)), ((), ())), preferred_element_type=f32
        )
        bsum[...] += jnp.sum(grad.astype(f32), axis=0, keepdims=True)
        back = lax.dot_general(
            grad, weight[...], (((1,), (1,)), ((), ())), preferred_element_type=f32
        )
        mixed[span] = back.astype(bf16).reshape(step, edge, width)

    @pl.loop(0, chunks * (chunk // group))
    def _(g):
        for j in range(group):
            k = g * group + j
            product = lax.dot_general(
                held[k], mixed[tile_row[0, k]], (((0,), (0,)), ((), ())),
                preferred_element_type=f32,
            )
            target = jnp.where(k < total, tile_col[0, k], ext)
            backward[target] += product

    def out_copy(b):
        span = pl.ds(b * step, step)
        return pltpu.make_async_copy(spread.at[span], own_grad.at[span], out_sem.at[b])

    @pl.loop(0, own // step)
    def _(b):
        span = pl.ds(b * step, step)
        spread[span] = backward[span].astype(bf16)
        out_copy(b).start()

    halo_grad[...] = backward[pl.ds(own, ext - own)].astype(bf16)
    pieces, piece_rows = weight_part.shape[:2]
    for p in range(pieces):
        weight_part[p] = wsum[pl.ds(p * piece_rows, piece_rows), :].astype(bf16)
    bias_part[...] = bsum[...]

    @pl.loop(0, own // step)
    def _(b):
        act_copy(b).wait()
        out_copy(b).wait()


def local_pass(n, tile_row, tile_col, tile_count, features, halo, tiles, cotangent, weight, bias):
    own, edge, width = features.shape
    ext = own + halo.shape[0]
    number = tiles.shape[0]
    chunk = math.gcd(number, CHUNK)
    steps = own // math.gcd(own, 4)
    anywhere = pl.BlockSpec(memory_space=pltpu.HBM)
    smem = pl.BlockSpec(memory_space=pltpu.SMEM)
    vmem = pl.BlockSpec(memory_space=VMEM)
    dma = pltpu.SemaphoreType.DMA
    return pl.pallas_call(
        local_kernel,
        out_shape=(
            jax.ShapeDtypeStruct(features.shape, bf16),
            jax.ShapeDtypeStruct(features.shape, bf16),
            jax.ShapeDtypeStruct(halo.shape, bf16),
            jax.ShapeDtypeStruct((n, width // n, width), bf16),
            jax.ShapeDtypeStruct((1, width), f32),
        ),
        in_specs=[smem] * 3 + [anywhere] * 4 + [vmem] * 2,
        out_specs=(anywhere, anywhere, vmem, vmem, vmem),
        scratch_shapes=[
            VMEM((ext, edge, width), bf16),
            VMEM(tiles.shape, bf16),
            VMEM(features.shape, bf16),
            VMEM(features.shape, bf16),
            VMEM(features.shape, bf16),
            VMEM((own + 1, edge, width), f32),
            VMEM((ext + 1, edge, width), f32),
            VMEM(features.shape, bf16),
            VMEM((width, width), f32),
            VMEM((1, width), f32),
            dma((2,)),
            dma((number // chunk,)),
            dma,
            dma((steps,)),
            dma((steps,)),
        ],
        compiler_params=pltpu.CompilerParams(vmem_limit_bytes=56 * 1024 * 1024),
        name="local_pass",
    )(tile_row, tile_col, tile_count, features, halo, tiles, cotangent, weight, bias)


def return_kernel(
    n, scale, halo_ref, weight_ref, bias_ref, halo_in, pieces_in, bsum_ref,
    halo_land, weight_in, bias_in, piece, pieces_land,
    halo_s, halo_r, weight_s, weight_r, bias_s, bias_r, piece_s, piece_r,
):
    me = lax.axis_index("dom")
    barrier = greet(n, me)
    pl.semaphore_wait(barrier, n - 1)
    halo_copy = functools.partial(push, n, me, lambda p: halo_ref.at[p], halo_land, halo_s, halo_r)
    weight_copy = functools.partial(
        push, n, me, lambda p: weight_ref.at[p], weight_in, weight_s, weight_r
    )
    bias_copy = functools.partial(push, n, me, lambda p: bias_ref, bias_in, bias_s, bias_r)
    piece_copy = functools.partial(push, n, me, lambda p: piece, pieces_land, piece_s, piece_r)

    def over(step):
        def turn(i, carry):
            step(i)
            return carry

        lax.fori_loop(1, n, turn, 0)

    def first(i):
        weight_copy(i).start()
        bias_copy(i).start()

    over(first)
    over(lambda i: halo_copy(i).start())
    weight_in[me] = weight_ref[me]
    bias_in[me] = bias_ref[...]
    halo_land[me] = halo_ref[me]
    over(lambda i: weight_copy(i).wait())
    piece[...] = (jnp.sum(weight_in[...].astype(f32), axis=0) * scale).astype(bf16)
    over(lambda i: piece_copy(i).start())
    pieces_land[me] = piece[...]
    over(lambda i: bias_copy(i).wait())
    bsum_ref[...] = jnp.sum(bias_in[...], axis=0) * scale
    over(lambda i: halo_copy(i).wait())
    halo_in[...] = halo_land[...]
    over(lambda i: piece_copy(i).wait())
    pieces_in[...] = pieces_land[...]


def exchange_return(n, scale, halo_grad, weight_part, bias_part):
    vmem = pl.BlockSpec(memory_space=VMEM)
    return pl.pallas_call(
        functools.partial(return_kernel, n, scale),
        out_shape=(
            jax.ShapeDtypeStruct(halo_grad.shape, bf16),
            jax.ShapeDtypeStruct(weight_part.shape, bf16),
            jax.ShapeDtypeStruct(bias_part.shape, f32),
        ),
        in_specs=[vmem] * 3,
        out_specs=(vmem,) * 3,
        scratch_shapes=[
            VMEM(halo_grad.shape, bf16),
            VMEM(weight_part.shape, bf16),
            VMEM((n,) + bias_part.shape, f32),
            VMEM(weight_part.shape[1:], bf16),
            VMEM(weight_part.shape, bf16),
        ]
        + [pltpu.SemaphoreType.DMA((n,))] * 8,
        compiler_params=pltpu.CompilerParams(collective_id=1, has_side_effects=True),
        name="return_exchange",
    )(halo_grad, weight_part, bias_part)


def final_kernel(
    chosen_ref, returned, pieces, bias_sum, own_hbm, out_hbm, wsum_ref, bsum_ref,
    own, out, load_sem, out_sem,
):
    rows = own.shape[0]
    step = math.gcd(rows, 512)
    spans = [pl.ds(c * step, step) for c in range(rows // step)]
    loads = [
        pltpu.make_async_copy(own_hbm.at[span], own.at[span], load_sem.at[c])
        for c, span in enumerate(spans)
    ]
    for load in loads:
        load.start()
    wsum_ref[...] = pieces[...].astype(f32)
    bsum_ref[...] = bias_sum[...]
    slots = chosen_ref.shape[1]
    ids = lax.broadcasted_iota(jnp.int32, (step, slots), 0)
    outs = []
    for c, span in enumerate(spans):
        hot = jnp.where(ids == chosen_ref[...] - c * step, 1.0, 0.0).astype(bf16)
        collected = jnp.dot(hot, returned[...], preferred_element_type=f32)
        loads[c].wait()
        out[span, :] = (own[span, :].astype(f32) + collected).astype(bf16)
        outs.append(pltpu.make_async_copy(out.at[span], out_hbm.at[span], out_sem.at[c]))
        outs[c].start()
    for copy in outs:
        copy.wait()


def final_pass(chosen, returned, pieces, bias_sum, own_grad):
    rows, width = own_grad.shape
    vmem = pl.BlockSpec(memory_space=VMEM)
    hbm = pl.BlockSpec(memory_space=pltpu.HBM)
    steps = rows // math.gcd(rows, 512)
    return pl.pallas_call(
        final_kernel,
        out_shape=(
            jax.ShapeDtypeStruct(own_grad.shape, bf16),
            jax.ShapeDtypeStruct(pieces.shape, f32),
            jax.ShapeDtypeStruct(bias_sum.shape, f32),
        ),
        in_specs=[vmem] * 4 + [hbm],
        out_specs=(hbm, vmem, vmem),
        scratch_shapes=[
            VMEM(own_grad.shape, bf16),
            VMEM(own_grad.shape, bf16),
            pltpu.SemaphoreType.DMA((steps,)),
            pltpu.SemaphoreType.DMA((steps,)),
        ],
        compiler_params=pltpu.CompilerParams(vmem_limit_bytes=60 * 1024 * 1024),
        name="final_pass",
    )(chosen, returned, pieces, bias_sum, own_grad)


def body(
    features, weight, bias_vector, tile_values, tile_row, tile_col, tile_count, send_rows,
    send_count, cotangent,
):
    rows, width = features.shape
    n = lax.axis_size("dom")
    slot_count = send_rows.shape[2]
    edge = tile_values.shape[1]
    slots = n * slot_count
    send_rows = jnp.swapaxes(send_rows, 1, 2).reshape(slot_count, n)
    halo, chosen = exchange_gather(n, send_count, send_rows, features)
    blocks = lambda a: a.reshape(-1, edge, width)
    activation, own_grad, halo_grad, weight_part, bias_part = local_pass(
        n, tile_row, tile_col, tile_count, blocks(features), blocks(halo), tile_values,
        blocks(cotangent), weight, bias_vector.reshape(1, width),
    )
    scale = float(rows * n) ** (-0.5)
    returned, pieces, bias_sum = exchange_return(
        n, scale, halo_grad.reshape(n, slot_count, width), weight_part, bias_part
    )
    grad_features, weight_sum, bias_sum = final_pass(
        chosen, returned.reshape(slots, width), pieces.reshape(width, width), bias_sum,
        own_grad.reshape(rows, width),
    )
    return (activation.reshape(rows, width), grad_features, weight_sum, bias_sum.reshape(width))


def solution(mesh):
    return jax.shard_map(
        body,
        mesh=mesh,
        in_specs=(
            P("dom", None),
            P(),
            P(),
            P("dom", None, None),
            P("dom", None),
            P("dom", None),
            P("dom"),
            P("dom", None, None),
            P("dom", None),
            P("dom", None),
        ),
        out_specs=(P("dom", None), P("dom", None), P(), P()),
        check_vma=False,
    )
```

```python
import functools
import math

import jax
import jax.numpy as jnp
from jax import lax
from jax.experimental import pallas as pl
from jax.experimental.pallas import tpu as pltpu
from jax.sharding import PartitionSpec as P

MESH = pl.DeviceIdType.MESH
VMEM = pltpu.VMEM
f32 = jnp.float32
bf16 = jnp.bfloat16


def greet(n, me):
    barrier = pltpu.get_barrier_semaphore()

    def signal(i, carry):
        pl.semaphore_signal(
            barrier, inc=1, device_id=(lax.rem(me + i, n),), device_id_type=MESH
        )
        return carry

    lax.fori_loop(1, n, signal, 0)
    return barrier


def push(n, me, src, dst, send_sem, recv_sem, i):
    peer = lax.rem(me + i, n)
    return pltpu.make_async_remote_copy(
        src_ref=src(peer),
        dst_ref=dst.at[me],
        send_sem=send_sem.at[i],
        recv_sem=recv_sem.at[i],
        device_id=(peer,),
        device_id_type=MESH,
    )


LANES = 128
UNROLL = 8
CHUNK = 16
MIB = 1024 * 1024


def padded(size, step):
    return (size + step - 1) // step * step


def bits(size):
    return max(1, (size - 1).bit_length())


def pair_slots(number, keys):
    return padded((number + keys + 1) // 2, UNROLL)


def table_width(number, own):
    return padded(max(2 * pair_slots(number, own), number), LANES)


def down(row):
    return jnp.broadcast_to(row, (LANES, row.shape[1])).T


def iota(shape, dim):
    return lax.broadcasted_iota(jnp.int32, shape, dim)


def place(position, code, default, width):
    position, code = down(position), down(code - default)
    found = []
    for start in range(0, width, LANES):
        hit = position == iota(position.shape, 1) + start
        found.append(jnp.sum(jnp.where(hit, code, 0), axis=0, keepdims=True) + default)
    return jnp.concatenate(found, axis=1)


def wide_columns(columns, width):
    return jnp.concatenate([columns] * (width // LANES), axis=1)


def rank_of(same, valid):
    number = valid.shape[1]
    before = iota((number, number), 0) < iota((number, number), 1)
    taken = jnp.where(before & same, wide_columns(down(valid), number), 0)
    return jnp.sum(taken, axis=0, keepdims=True)


def pair_table(key, other, valid, zero, slots, width):
    number = key.shape[1]
    key_down, valid_down = down(key), down(valid)
    lane = iota((number, LANES), 1)
    count = jnp.sum(jnp.where(key_down == lane, valid_down, 0), axis=0, keepdims=True)
    pairs = (count + 1) // 2
    pairs_down = down(pairs)
    square = (LANES, LANES)
    upto = iota(square, 0) <= iota(square, 1)
    ends = jnp.sum(jnp.where(upto, pairs_down, 0), axis=0, keepdims=True)
    last = jnp.where(count > 0, ends - 1, slots)
    same = wide_columns(key_down, number) == key
    rank = rank_of(same, valid)
    lower = iota((LANES, number), 0) < key
    base = jnp.sum(jnp.where(lower, wide_columns(pairs_down, number), 0), axis=0, keepdims=True)
    position = jnp.where(valid > 0, 2 * base + rank, -1)
    tile = iota((1, number), 1)
    low, high = bits(number), bits(zero + 1)
    first = jnp.where(rank == 0, 1, 0)
    code = tile + other * (1 << low) + first * (1 << (low + high))
    return place(position, code, zero << low, width), last


def fill_table(table, row, col, count, own, ext):
    number = row.shape[1]
    width = table.shape[1]
    slots = pair_slots(number, own)
    used = iota((1, number), 1) < count
    mine = jnp.where(used & (col < own), 1, 0)
    far = jnp.where(used & (col >= own), 1, 0)
    table[...] = jnp.zeros_like(table)
    order, last = pair_table(row, col, mine, own, slots, width)
    table[0:1, :] = order
    table[1:2, :LANES] = last
    order, last = pair_table(col, row, mine, own, slots, width)
    table[2:3, :] = order
    table[3:4, :LANES] = last
    every = iota((number, number), 0) >= 0
    rank = rank_of(every, far)
    low, high = bits(number), bits(ext)
    code = iota((1, number), 1) + (col + row * (1 << high)) * (1 << low)
    position = jnp.where(far > 0, rank, -1)
    table[4:5, :] = place(position, code, (own + (own << high)) << low, width)
    total = jnp.sum(down(far), axis=0, keepdims=True)
    table[5:6, :LANES] = total


def choose(n, count_ref, rows_ref, wide):
    slots, lanes = rows_ref.shape[0], wide.shape[1]
    slot = iota((slots, 1), 0)
    for p in range(n):
        column = jnp.where(slot < count_ref[0, p], rows_ref[:, p : p + 1], -1)
        wide[pl.ds(p * slots, slots), :] = jnp.broadcast_to(column, (slots, lanes))


def run_pairs(table, line, number, zero, held, source, transposed, running, kept):
    low, high = bits(number), bits(zero + 1)
    slots = kept.shape[0] - 1
    kept[slots] = jnp.zeros(kept.shape[1:], kept.dtype)
    running[...] = jnp.zeros_like(running)
    axis = 0 if transposed else 1

    def turn(g, carry):
        total = running[...]
        for j in range(UNROLL):
            p = g * UNROLL + j
            one, two = table[line, 2 * p], table[line, 2 * p + 1]
            tiles = [held[code & ((1 << low) - 1)] for code in (one, two)]
            blocks = [source[(code >> low) & ((1 << high) - 1)] for code in (one, two)]
            product = lax.dot_general(
                jnp.concatenate(tiles, axis=axis), jnp.concatenate(blocks, axis=0),
                (((axis,), (0,)), ((), ())), preferred_element_type=f32,
            )
            keep = (1 - (one >> (low + high))).astype(f32)
            total = total * keep + product
            kept[p] = total.astype(kept.dtype)
        running[...] = total
        return carry

    lax.fori_loop(0, slots // UNROLL, turn, 0)


def gather_kernel(
    n, count_ref, tile_count, rows_ref, row_ref, col_ref, features_hbm, tiles_hbm,
    halo_ref, chosen_ref, table_ref, held, agg_ref,
    source, wide, total, sent, landed, table, running, kept,
    send_sem, recv_sem, load_sem, tile_sem, table_sem,
):
    me = lax.axis_index("dom")
    own = features_hbm.shape[0]
    edge, width = features_hbm.shape[1:]
    number = tiles_hbm.shape[0]
    step = math.gcd(own, 4)
    loads = []
    for c in range(own // step):
        span = pl.ds(c * step, step)
        loads.append(pltpu.make_async_copy(features_hbm.at[span], source.at[span], load_sem.at[c]))
        loads[c].start()
    chunk = math.gcd(number, CHUNK)
    tile_loads = []
    for c in range(number // chunk):
        span = pl.ds(c * chunk, chunk)
        tile_loads.append(pltpu.make_async_copy(tiles_hbm.at[span], held.at[span], tile_sem.at[c]))
        tile_loads[c].start()
    barrier = greet(n, me)
    choose(n, count_ref, rows_ref, wide)
    lane = iota(wide.shape, 1)
    for c in range(own // step):
        hot = jnp.concatenate(
            [
                jnp.where(wide[...] == lane + (c * step * edge + j), 1.0, 0.0).astype(bf16)
                for j in range(0, step * edge, LANES)
            ],
            axis=1,
        )
        loads[c].wait()
        block = source[pl.ds(c * step, step)].reshape(step * edge, width)
        part = jnp.dot(hot, block, preferred_element_type=f32)
        if c == 0:
            total[...] = part
        else:
            total[...] += part
    sent[...] = total[...].astype(bf16).reshape(sent.shape)
    pl.semaphore_wait(barrier, n - 1)
    copy = functools.partial(push, n, me, lambda p: sent.at[p], landed, send_sem, recv_sem)

    def start(i, carry):
        copy(i).start()
        return carry

    def finish(i, carry):
        copy(i).wait()
        return carry

    lax.fori_loop(1, n, start, 0)
    landed[me] = sent[me]
    ext = own + wide.shape[0] // edge
    fill_table(table_ref, row_ref[...], col_ref[...], tile_count[0], own, ext)
    move = pltpu.make_async_copy(table_ref, table, table_sem)
    move.start()
    chosen_ref[...] = wide[...].T[:1, :]
    source[own] = jnp.zeros((edge, width), bf16)
    for load in tile_loads:
        load.wait()
    move.wait()
    run_pairs(table, 0, number, own, held, source, False, running, kept)

    def pick(r, carry):
        agg_ref[r] = kept[table[1, r]]
        return carry

    lax.fori_loop(0, own, pick, 0)
    lax.fori_loop(1, n, finish, 0)
    halo_ref[...] = landed[...]


def exchange_gather(n, send_count, tile_count, send_rows, tile_row, tile_col, features, tiles):
    own, edge, width = features.shape
    number = tiles.shape[0]
    slot_count = send_rows.shape[0]
    slots = n * slot_count
    block = (n, slot_count, width)
    pairs = pair_slots(number, own)
    table = (8, table_width(number, own))
    vmem = pl.BlockSpec(memory_space=VMEM)
    smem = pl.BlockSpec(memory_space=pltpu.SMEM)
    hbm = pl.BlockSpec(memory_space=pltpu.HBM)
    dma = pltpu.SemaphoreType.DMA
    return pl.pallas_call(
        functools.partial(gather_kernel, n),
        out_shape=(
            jax.ShapeDtypeStruct(block, bf16),
            jax.ShapeDtypeStruct((1, slots), jnp.int32),
            jax.ShapeDtypeStruct(table, jnp.int32),
            jax.ShapeDtypeStruct(tiles.shape, bf16),
            jax.ShapeDtypeStruct(features.shape, bf16),
        ),
        in_specs=[smem, smem, vmem, vmem, vmem, hbm, hbm],
        out_specs=(vmem,) * 5,
        scratch_shapes=[
            VMEM((own + 1, edge, width), bf16),
            VMEM((slots, LANES), jnp.int32),
            VMEM((slots, width), f32),
            VMEM(block, bf16),
            VMEM(block, bf16),
            pltpu.SMEM(table, jnp.int32),
            VMEM((edge, width), f32),
            VMEM((pairs + 1, edge, width), bf16),
            dma((n,)),
            dma((n,)),
            dma((own // math.gcd(own, 4),)),
            dma((number // math.gcd(number, CHUNK),)),
            dma,
        ],
        compiler_params=pltpu.CompilerParams(
            collective_id=0, has_side_effects=True, vmem_limit_bytes=24 * MIB + slots * 8192
        ),
        name="gather_exchange",
    )(send_count, tile_count, send_rows, tile_row, tile_col, features, tiles)


GROUP = 4


def local_kernel(
    table, aggregate, halo, held, cotangent, weight, bias,
    activation, mixed, halo_grad, weight_part, bias_part,
    cot, act, extra, spread, wsum, bsum, cot_sem, act_sem,
):
    own = aggregate.shape[0]
    edge, width = aggregate.shape[1:]
    number = held.shape[0]
    far = halo.shape[0]
    low, high = bits(number), bits(own + far)
    step = math.gcd(own, 4)
    steps = own // step
    cot_copies = []
    for b in range(steps):
        span = pl.ds(b * step, step)
        cot_copies.append(pltpu.make_async_copy(cotangent.at[span], cot.at[span], cot_sem.at[b]))
        cot_copies[b].start()

    @pl.loop(0, own + 1)
    def _(r):
        extra[r] = jnp.zeros(extra.shape[1:], f32)

    spread[...] = jnp.zeros_like(spread)
    groups = (table[5, 0] + GROUP - 1) // GROUP

    def parts(s):
        code = table[4, s]
        return (
            code & ((1 << low) - 1), ((code >> low) & ((1 << high) - 1)) - own,
            code >> (low + high),
        )

    @pl.loop(0, groups)
    def _(g):
        for j in range(GROUP):
            k, col, row = parts(g * GROUP + j)
            extra[row] += jnp.dot(held[k], halo[col], preferred_element_type=f32)

    wsum[...] = jnp.zeros_like(wsum)
    bsum[...] = jnp.zeros_like(bsum)
    act_copies = []
    for b in range(steps):
        span = pl.ds(b * step, step)
        act_copies.append(pltpu.make_async_copy(act.at[span], activation.at[span], act_sem.at[b]))
        agg = (aggregate[span].astype(f32) + extra[span]).astype(bf16).reshape(step * edge, width)
        linear = jnp.dot(agg, weight[...], preferred_element_type=f32) + bias[...]
        sig = 0.5 * jnp.tanh(0.5 * linear) + 0.5
        value = linear * sig
        act[span] = value.astype(bf16).reshape(step, edge, width)
        act_copies[b].start()
        slope = sig + value * (1.0 - sig)
        cot_copies[b].wait()
        grad = (cot[span].reshape(step * edge, width).astype(f32) * slope).astype(bf16)
        wsum[...] += lax.dot_general(
            agg, grad, (((0,), (0,)), ((), ())), preferred_element_type=f32
        )
        bsum[...] += jnp.sum(grad.astype(f32), axis=0, keepdims=True)
        back = lax.dot_general(
            grad, weight[...], (((1,), (1,)), ((), ())), preferred_element_type=f32
        )
        mixed[span] = back.astype(bf16).reshape(step, edge, width)
    mixed[own] = jnp.zeros((edge, width), bf16)

    @pl.loop(0, groups)
    def _(g):
        for j in range(GROUP):
            s = g * GROUP + j
            k, col, row = parts(s)
            target = jnp.where(s < table[5, 0], col, far)
            spread[target] += lax.dot_general(
                held[k], mixed[row], (((0,), (0,)), ((), ())), preferred_element_type=f32
            )

    halo_grad[...] = spread[pl.ds(0, far)].astype(bf16)
    pieces, piece_rows = weight_part.shape[:2]
    for p in range(pieces):
        weight_part[p] = wsum[pl.ds(p * piece_rows, piece_rows), :].astype(bf16)
    bias_part[...] = bsum[...]
    for copy in act_copies:
        copy.wait()


def local_pass(n, table, aggregate, halo, held, cotangent, weight, bias):
    own, edge, width = aggregate.shape
    steps = own // math.gcd(own, 4)
    hbm = pl.BlockSpec(memory_space=pltpu.HBM)
    smem = pl.BlockSpec(memory_space=pltpu.SMEM)
    vmem = pl.BlockSpec(memory_space=VMEM)
    dma = pltpu.SemaphoreType.DMA
    return pl.pallas_call(
        local_kernel,
        out_shape=(
            jax.ShapeDtypeStruct(aggregate.shape, bf16),
            jax.ShapeDtypeStruct((own + 1, edge, width), bf16),
            jax.ShapeDtypeStruct(halo.shape, bf16),
            jax.ShapeDtypeStruct((n, width // n, width), bf16),
            jax.ShapeDtypeStruct((1, width), f32),
        ),
        in_specs=[smem, vmem, vmem, vmem, hbm, vmem, vmem],
        out_specs=(hbm, vmem, vmem, vmem, vmem),
        scratch_shapes=[
            VMEM(aggregate.shape, bf16),
            VMEM(aggregate.shape, bf16),
            VMEM((own + 1, edge, width), f32),
            VMEM((halo.shape[0] + 1, edge, width), f32),
            VMEM((width, width), f32),
            VMEM((1, width), f32),
            dma((steps,)),
            dma((steps,)),
        ],
        compiler_params=pltpu.CompilerParams(vmem_limit_bytes=24 * MIB + halo.size * 16),
        name="local_pass",
    )(table, aggregate, halo, held, cotangent, weight, bias)


def return_kernel(
    n, scale, table, held, mixed, halo_ref, weight_ref, bias_ref,
    halo_in, pieces_in, bsum_ref, own_grad,
    halo_land, weight_in, bias_in, piece, pieces_land, running, kept,
    halo_s, halo_r, weight_s, weight_r, bias_s, bias_r, piece_s, piece_r,
):
    me = lax.axis_index("dom")
    barrier = greet(n, me)
    halo_copy = functools.partial(push, n, me, lambda p: halo_ref.at[p], halo_land, halo_s, halo_r)
    weight_copy = functools.partial(
        push, n, me, lambda p: weight_ref.at[p], weight_in, weight_s, weight_r
    )
    bias_copy = functools.partial(push, n, me, lambda p: bias_ref, bias_in, bias_s, bias_r)
    piece_copy = functools.partial(push, n, me, lambda p: piece, pieces_land, piece_s, piece_r)

    def over(step):
        def turn(i, carry):
            step(i)
            return carry

        lax.fori_loop(1, n, turn, 0)

    def first(i):
        weight_copy(i).start()
        bias_copy(i).start()

    pl.semaphore_wait(barrier, n - 1)
    over(first)
    over(lambda i: halo_copy(i).start())
    weight_in[me] = weight_ref[me]
    bias_in[me] = bias_ref[...]
    halo_land[me] = halo_ref[me]
    number = held.shape[0]
    own = mixed.shape[0] - 1
    run_pairs(table, 2, number, own, held, mixed, True, running, kept)
    over(lambda i: weight_copy(i).wait())
    piece[...] = (jnp.sum(weight_in[...].astype(f32), axis=0) * scale).astype(bf16)
    over(lambda i: piece_copy(i).start())
    pieces_land[me] = piece[...]

    def pick(c, carry):
        own_grad[c] = kept[table[3, c]]
        return carry

    lax.fori_loop(0, own, pick, 0)
    over(lambda i: bias_copy(i).wait())
    bsum_ref[...] = jnp.sum(bias_in[...], axis=0) * scale
    over(lambda i: halo_copy(i).wait())
    halo_in[...] = halo_land[...]
    over(lambda i: piece_copy(i).wait())
    pieces_in[...] = pieces_land[...]


def exchange_return(n, scale, table, held, mixed, halo_grad, weight_part, bias_part):
    vmem = pl.BlockSpec(memory_space=VMEM)
    smem = pl.BlockSpec(memory_space=pltpu.SMEM)
    edge, width = mixed.shape[1:]
    own = mixed.shape[0] - 1
    pairs = pair_slots(held.shape[0], own)
    return pl.pallas_call(
        functools.partial(return_kernel, n, scale),
        out_shape=(
            jax.ShapeDtypeStruct(halo_grad.shape, bf16),
            jax.ShapeDtypeStruct(weight_part.shape, bf16),
            jax.ShapeDtypeStruct(bias_part.shape, f32),
            jax.ShapeDtypeStruct((own, edge, width), bf16),
        ),
        in_specs=[smem] + [vmem] * 5,
        out_specs=(vmem,) * 4,
        scratch_shapes=[
            VMEM(halo_grad.shape, bf16),
            VMEM(weight_part.shape, bf16),
            VMEM((n,) + bias_part.shape, f32),
            VMEM(weight_part.shape[1:], bf16),
            VMEM(weight_part.shape, bf16),
            VMEM((edge, width), f32),
            VMEM((pairs + 1, edge, width), bf16),
        ]
        + [pltpu.SemaphoreType.DMA((n,))] * 8,
        compiler_params=pltpu.CompilerParams(
            collective_id=1, has_side_effects=True,
            vmem_limit_bytes=20 * MIB + halo_grad.size * 16,
        ),
        name="return_exchange",
    )(table, held, mixed, halo_grad, weight_part, bias_part)


def final_kernel(
    chosen_ref, returned, pieces, bias_sum, own, out_hbm, wsum_hbm, bsum_hbm,
    out, wsum, bsum, out_sem, small_sem,
):
    rows = own.shape[0]
    step = math.gcd(rows, 512)
    spans = [pl.ds(c * step, step) for c in range(rows // step)]
    wsum[...] = pieces[...].astype(f32)
    bsum[...] = bias_sum[...]
    outs = [
        pltpu.make_async_copy(wsum, wsum_hbm, small_sem.at[0]),
        pltpu.make_async_copy(bsum, bsum_hbm, small_sem.at[1]),
    ]
    for copy in outs:
        copy.start()
    slots = chosen_ref.shape[1]
    ids = iota((step, slots), 0)
    for c, span in enumerate(spans):
        hot = jnp.where(ids == chosen_ref[...] - c * step, 1.0, 0.0).astype(bf16)
        collected = jnp.dot(hot, returned[...], preferred_element_type=f32)
        out[span, :] = (own[span, :].astype(f32) + collected).astype(bf16)
        copy = pltpu.make_async_copy(out.at[span], out_hbm.at[span], out_sem.at[c])
        copy.start()
        outs.append(copy)
    for copy in outs:
        copy.wait()


def final_pass(chosen, returned, pieces, bias_sum, own_grad):
    rows, width = own_grad.shape
    vmem = pl.BlockSpec(memory_space=VMEM)
    hbm = pl.BlockSpec(memory_space=pltpu.HBM)
    steps = rows // math.gcd(rows, 512)
    return pl.pallas_call(
        final_kernel,
        out_shape=(
            jax.ShapeDtypeStruct(own_grad.shape, bf16),
            jax.ShapeDtypeStruct(pieces.shape, f32),
            jax.ShapeDtypeStruct(bias_sum.shape, f32),
        ),
        in_specs=[vmem] * 5,
        out_specs=(hbm,) * 3,
        scratch_shapes=[
            VMEM(own_grad.shape, bf16),
            VMEM(pieces.shape, f32),
            VMEM(bias_sum.shape, f32),
            pltpu.SemaphoreType.DMA((steps,)),
            pltpu.SemaphoreType.DMA((2,)),
        ],
        compiler_params=pltpu.CompilerParams(vmem_limit_bytes=12 * MIB + returned.size * 32),
        name="final_pass",
    )(chosen, returned, pieces, bias_sum, own_grad)


def body(
    features, weight, bias_vector, tile_values, tile_row, tile_col, tile_count, send_rows,
    send_count, cotangent,
):
    rows, width = features.shape
    n = lax.axis_size("dom")
    slot_count = send_rows.shape[2]
    edge = tile_values.shape[1]
    slots = n * slot_count
    send_rows = jnp.swapaxes(send_rows, 1, 2).reshape(slot_count, n)
    blocks = lambda a: a.reshape(-1, edge, width)
    halo, chosen, table, held, aggregate = exchange_gather(
        n, send_count, tile_count, send_rows, tile_row, tile_col, blocks(features), tile_values
    )
    activation, mixed, halo_grad, weight_part, bias_part = local_pass(
        n, table, aggregate, blocks(halo), held, blocks(cotangent), weight,
        bias_vector.reshape(1, width),
    )
    scale = float(rows * n) ** (-0.5)
    returned, pieces, bias_sum, own_grad = exchange_return(
        n, scale, table, held, mixed, halo_grad.reshape(n, slot_count, width), weight_part,
        bias_part,
    )
    grad_features, weight_sum, bias_sum = final_pass(
        chosen, returned.reshape(slots, width), pieces.reshape(width, width), bias_sum,
        own_grad.reshape(rows, width),
    )
    return (activation.reshape(rows, width), grad_features, weight_sum, bias_sum.reshape(width))


def solution(mesh):
    return jax.shard_map(
        body,
        mesh=mesh,
        in_specs=(
            P("dom", None),
            P(),
            P(),
            P("dom", None, None),
            P("dom", None),
            P("dom", None),
            P("dom"),
            P("dom", None, None),
            P("dom", None),
            P("dom", None),
        ),
        out_specs=(P("dom", None), P("dom", None), P(), P()),
        check_vma=False,
    )
```

```python
import functools
import math

import jax
import jax.numpy as jnp
from jax import lax
from jax.experimental import pallas as pl
from jax.experimental.pallas import tpu as pltpu
from jax.sharding import PartitionSpec as P

MESH = pl.DeviceIdType.MESH
VMEM = pltpu.VMEM
f32 = jnp.float32
bf16 = jnp.bfloat16


def greet(n, me):
    barrier = pltpu.get_barrier_semaphore()

    def signal(i, carry):
        pl.semaphore_signal(
            barrier, inc=1, device_id=(lax.rem(me + i, n),), device_id_type=MESH
        )
        return carry

    lax.fori_loop(1, n, signal, 0)
    return barrier


def push(n, me, src, dst, send_sem, recv_sem, i):
    peer = lax.rem(me + i, n)
    return pltpu.make_async_remote_copy(
        src_ref=src(peer),
        dst_ref=dst.at[me],
        send_sem=send_sem.at[i],
        recv_sem=recv_sem.at[i],
        device_id=(peer,),
        device_id_type=MESH,
    )


LANES = 128
UNROLL = 8
NEAR = 8
CHUNK = 16
MIB = 1024 * 1024


def padded(size, step):
    return (size + step - 1) // step * step


def bits(size):
    return max(1, (size - 1).bit_length())


def pair_slots(number, keys):
    return padded((number + keys + 1) // 2, UNROLL)


def table_width(number, own):
    return padded(max(2 * pair_slots(number, own), number), LANES)


def down(row):
    return jnp.broadcast_to(row, (LANES, row.shape[1])).T


def iota(shape, dim):
    return lax.broadcasted_iota(jnp.int32, shape, dim)


def place(position, code, default, width):
    position, code = down(position), down(code - default)
    found = []
    for start in range(0, width, LANES):
        hit = position == iota(position.shape, 1) + start
        found.append(jnp.sum(jnp.where(hit, code, 0), axis=0, keepdims=True) + default)
    return jnp.concatenate(found, axis=1)


def wide_columns(columns, width):
    return jnp.concatenate([columns] * (width // LANES), axis=1)


def rank_of(same, valid):
    number = valid.shape[1]
    before = iota((number, number), 0) < iota((number, number), 1)
    taken = jnp.where(before & same, wide_columns(down(valid), number), 0)
    return jnp.sum(taken, axis=0, keepdims=True)


def pair_table(key, other, valid, zero, slots, width):
    number = key.shape[1]
    key_down, valid_down = down(key), down(valid)
    lane = iota((number, LANES), 1)
    count = jnp.sum(jnp.where(key_down == lane, valid_down, 0), axis=0, keepdims=True)
    pairs = (count + 1) // 2
    pairs_down = down(pairs)
    square = (LANES, LANES)
    upto = iota(square, 0) <= iota(square, 1)
    ends = jnp.sum(jnp.where(upto, pairs_down, 0), axis=0, keepdims=True)
    last = jnp.where(count > 0, ends - 1, slots)
    same = wide_columns(key_down, number) == key
    rank = rank_of(same, valid)
    lower = iota((LANES, number), 0) < key
    base = jnp.sum(jnp.where(lower, wide_columns(pairs_down, number), 0), axis=0, keepdims=True)
    position = jnp.where(valid > 0, 2 * base + rank, -1)
    tile = iota((1, number), 1)
    low, high = bits(number), bits(zero + 1)
    first = jnp.where(rank == 0, 1, 0)
    code = tile + other * (1 << low) + first * (1 << (low + high))
    return place(position, code, zero << low, width), last


def fill_table(table, row, col, count, own, ext):
    number = row.shape[1]
    width = table.shape[1]
    slots = pair_slots(number, own)
    used = iota((1, number), 1) < count
    mine = jnp.where(used & (col < own), 1, 0)
    far = jnp.where(used & (col >= own), 1, 0)
    table[...] = jnp.zeros_like(table)
    order, last = pair_table(row, col, mine, own, slots, width)
    table[0:1, :] = order
    table[1:2, :LANES] = last
    order, last = pair_table(col, row, mine, own, slots, width)
    table[2:3, :] = order
    table[3:4, :LANES] = last
    every = iota((number, number), 0) >= 0
    rank = rank_of(every, far)
    low, high = bits(number), bits(ext)
    code = iota((1, number), 1) + (col + row * (1 << high)) * (1 << low)
    position = jnp.where(far > 0, rank, -1)
    table[4:5, :] = place(position, code, (own + (own << high)) << low, width)
    total = jnp.sum(down(far), axis=0, keepdims=True)
    table[5:6, :LANES] = total


def choose(n, count_ref, rows_ref, wide):
    slots, lanes = rows_ref.shape[0], wide.shape[1]
    slot = iota((slots, 1), 0)
    for p in range(n):
        column = jnp.where(slot < count_ref[0, p], rows_ref[:, p : p + 1], -1)
        wide[pl.ds(p * slots, slots), :] = jnp.broadcast_to(column, (slots, lanes))


def run_pairs(table, line, number, zero, held, source, transposed, running, kept, begin, end):
    low, high = bits(number), bits(zero + 1)
    slots = kept.shape[0] - 1
    if begin == 0:
        kept[slots] = jnp.zeros(kept.shape[1:], kept.dtype)
        running[...] = jnp.zeros_like(running)
    axis = 0 if transposed else 1

    def turn(g, carry):
        total = running[...]
        for j in range(UNROLL):
            p = g * UNROLL + j
            one, two = table[line, 2 * p], table[line, 2 * p + 1]
            tiles = [held[code & ((1 << low) - 1)] for code in (one, two)]
            blocks = [source[(code >> low) & ((1 << high) - 1)] for code in (one, two)]
            product = lax.dot_general(
                jnp.concatenate(tiles, axis=axis), jnp.concatenate(blocks, axis=0),
                (((axis,), (0,)), ((), ())), preferred_element_type=f32,
            )
            keep = (1 - (one >> (low + high))).astype(f32)
            total = total * keep + product
            kept[p] = total.astype(kept.dtype)
        running[...] = total
        return carry

    lax.fori_loop(begin, end, turn, 0)


def gather_kernel(
    n, tile_count, count_hbm, rows_hbm, row_hbm, col_hbm, features_hbm, tiles_hbm,
    halo_ref, chosen_ref, table_ref, held, agg_ref,
    count_ref, rows_ref, row_ref, col_ref,
    source, wide, total, sent, landed, table, running, kept,
    send_sem, recv_sem, load_sem, tile_sem, table_sem, small_sem,
):
    me = lax.axis_index("dom")
    own = features_hbm.shape[0]
    edge, width = features_hbm.shape[1:]
    number = tiles_hbm.shape[0]
    step = math.gcd(own, 4)
    smalls = [
        pltpu.make_async_copy(count_hbm, count_ref, small_sem.at[0]),
        pltpu.make_async_copy(rows_hbm, rows_ref, small_sem.at[1]),
        pltpu.make_async_copy(row_hbm, row_ref, small_sem.at[2]),
        pltpu.make_async_copy(col_hbm, col_ref, small_sem.at[3]),
    ]
    for copy in smalls:
        copy.start()
    loads = []
    for c in range(own // step):
        span = pl.ds(c * step, step)
        loads.append(pltpu.make_async_copy(features_hbm.at[span], source.at[span], load_sem.at[c]))
        loads[c].start()
    chunk = math.gcd(number, CHUNK)
    tile_loads = []
    for c in range(number // chunk):
        span = pl.ds(c * chunk, chunk)
        tile_loads.append(pltpu.make_async_copy(tiles_hbm.at[span], held.at[span], tile_sem.at[c]))
        tile_loads[c].start()
    barrier = greet(n, me)
    for copy in smalls:
        copy.wait()
    choose(n, count_ref, rows_ref, wide)
    lane = iota(wide.shape, 1)
    for c in range(own // step):
        hot = jnp.concatenate(
            [
                jnp.where(wide[...] == lane + (c * step * edge + j), 1.0, 0.0).astype(bf16)
                for j in range(0, step * edge, LANES)
            ],
            axis=1,
        )
        loads[c].wait()
        block = source[pl.ds(c * step, step)].reshape(step * edge, width)
        part = jnp.dot(hot, block, preferred_element_type=f32)
        if c == 0:
            total[...] = part
        else:
            total[...] += part
    sent[...] = total[...].astype(bf16).reshape(sent.shape)
    pl.semaphore_wait(barrier, n - 1)
    copy = functools.partial(push, n, me, lambda p: sent.at[p], landed, send_sem, recv_sem)

    def start(i, carry):
        copy(i).start()
        return carry

    def finish(i, carry):
        copy(i).wait()
        return carry

    lax.fori_loop(1, n, start, 0)
    landed[me] = sent[me]
    ext = own + wide.shape[0] // edge
    fill_table(table_ref, row_ref[...], col_ref[...], tile_count[0], own, ext)
    move = pltpu.make_async_copy(table_ref, table, table_sem)
    move.start()
    chosen_ref[...] = wide[...].T[:1, :]
    source[own] = jnp.zeros((edge, width), bf16)
    for load in tile_loads:
        load.wait()
    move.wait()
    turns = (kept.shape[0] - 1) // UNROLL
    run_pairs(table, 0, number, own, held, source, False, running, kept, 0, turns)

    def pick(r, carry):
        agg_ref[r] = kept[table[1, r]]
        return carry

    lax.fori_loop(0, own, pick, 0)
    lax.fori_loop(1, n, finish, 0)
    halo_ref[...] = landed[...]


def exchange_gather(n, send_count, tile_count, send_rows, tile_row, tile_col, features, tiles):
    own, edge, width = features.shape
    number = tiles.shape[0]
    slot_count = send_rows.shape[0]
    slots = n * slot_count
    block = (n, slot_count, width)
    pairs = pair_slots(number, own)
    table = (8, table_width(number, own))
    vmem = pl.BlockSpec(memory_space=VMEM)
    smem = pl.BlockSpec(memory_space=pltpu.SMEM)
    hbm = pl.BlockSpec(memory_space=pltpu.HBM)
    dma = pltpu.SemaphoreType.DMA
    return pl.pallas_call(
        functools.partial(gather_kernel, n),
        out_shape=(
            jax.ShapeDtypeStruct(block, bf16),
            jax.ShapeDtypeStruct((1, slots), jnp.int32),
            jax.ShapeDtypeStruct(table, jnp.int32),
            jax.ShapeDtypeStruct(tiles.shape, bf16),
            jax.ShapeDtypeStruct(features.shape, bf16),
        ),
        in_specs=[smem] + [hbm] * 6,
        out_specs=(vmem,) * 5,
        scratch_shapes=[
            pltpu.SMEM(send_count.shape, jnp.int32),
            VMEM(send_rows.shape, jnp.int32),
            VMEM(tile_row.shape, jnp.int32),
            VMEM(tile_col.shape, jnp.int32),
            VMEM((own + 1, edge, width), bf16),
            VMEM((slots, LANES), jnp.int32),
            VMEM((slots, width), f32),
            VMEM(block, bf16),
            VMEM(block, bf16),
            pltpu.SMEM(table, jnp.int32),
            VMEM((edge, width), f32),
            VMEM((pairs + 1, edge, width), bf16),
            dma((n,)),
            dma((n,)),
            dma((own // math.gcd(own, 4),)),
            dma((number // math.gcd(number, CHUNK),)),
            dma,
            dma((4,)),
        ],
        compiler_params=pltpu.CompilerParams(
            collective_id=0, has_side_effects=True, vmem_limit_bytes=24 * MIB + slots * 8192
        ),
        name="gather_exchange",
    )(
        tile_count,
        *[
            pltpu.with_memory_space_constraint(a, pltpu.HBM)
            for a in (send_count, send_rows, tile_row, tile_col, features, tiles)
        ],
    )


GROUP = 4


def local_kernel(
    table, aggregate, halo, held, cotangent, weight, bias,
    activation, mixed, halo_grad, weight_part, bias_part,
    cot, act, extra, spread, wsum, bsum, cot_sem, act_sem,
):
    own = aggregate.shape[0]
    edge, width = aggregate.shape[1:]
    number = held.shape[0]
    far = halo.shape[0]
    low, high = bits(number), bits(own + far)
    step = math.gcd(own, 4)
    steps = own // step
    cot_copies = []
    for b in range(steps):
        span = pl.ds(b * step, step)
        cot_copies.append(pltpu.make_async_copy(cotangent.at[span], cot.at[span], cot_sem.at[b]))
        cot_copies[b].start()

    @pl.loop(0, own + 1)
    def _(r):
        extra[r] = jnp.zeros(extra.shape[1:], f32)

    spread[...] = jnp.zeros_like(spread)
    groups = (table[5, 0] + GROUP - 1) // GROUP

    def parts(s):
        code = table[4, s]
        return (
            code & ((1 << low) - 1), ((code >> low) & ((1 << high) - 1)) - own,
            code >> (low + high),
        )

    @pl.loop(0, groups)
    def _(g):
        for j in range(GROUP):
            k, col, row = parts(g * GROUP + j)
            extra[row] += jnp.dot(held[k], halo[col], preferred_element_type=f32)

    wsum[...] = jnp.zeros_like(wsum)
    bsum[...] = jnp.zeros_like(bsum)
    act_copies = []
    for b in range(steps):
        span = pl.ds(b * step, step)
        act_copies.append(pltpu.make_async_copy(act.at[span], activation.at[span], act_sem.at[b]))
        agg = (aggregate[span].astype(f32) + extra[span]).astype(bf16).reshape(step * edge, width)
        linear = jnp.dot(agg, weight[...], preferred_element_type=f32) + bias[...]
        sig = 0.5 * jnp.tanh(0.5 * linear) + 0.5
        value = linear * sig
        act[span] = value.astype(bf16).reshape(step, edge, width)
        act_copies[b].start()
        slope = sig + value * (1.0 - sig)
        cot_copies[b].wait()
        grad = (cot[span].reshape(step * edge, width).astype(f32) * slope).astype(bf16)
        wsum[...] += lax.dot_general(
            agg, grad, (((0,), (0,)), ((), ())), preferred_element_type=f32
        )
        bsum[...] += jnp.sum(grad.astype(f32), axis=0, keepdims=True)
        back = lax.dot_general(
            grad, weight[...], (((1,), (1,)), ((), ())), preferred_element_type=f32
        )
        mixed[span] = back.astype(bf16).reshape(step, edge, width)
    mixed[own] = jnp.zeros((edge, width), bf16)

    @pl.loop(0, groups)
    def _(g):
        for j in range(GROUP):
            s = g * GROUP + j
            k, col, row = parts(s)
            target = jnp.where(s < table[5, 0], col, far)
            spread[target] += lax.dot_general(
                held[k], mixed[row], (((0,), (0,)), ((), ())), preferred_element_type=f32
            )

    halo_grad[...] = spread[pl.ds(0, far)].astype(bf16)
    pieces, piece_rows = weight_part.shape[:2]
    for p in range(pieces):
        weight_part[p] = wsum[pl.ds(p * piece_rows, piece_rows), :].astype(bf16)
    bias_part[...] = bsum[...]
    for copy in act_copies:
        copy.wait()


def local_pass(near, table, aggregate, halo, held, cotangent, weight, bias):
    own, edge, width = aggregate.shape
    steps = own // math.gcd(own, 4)
    hbm = pl.BlockSpec(memory_space=pltpu.HBM)
    smem = pl.BlockSpec(memory_space=pltpu.SMEM)
    vmem = pl.BlockSpec(memory_space=VMEM)
    dma = pltpu.SemaphoreType.DMA
    return pl.pallas_call(
        local_kernel,
        out_shape=(
            jax.ShapeDtypeStruct(aggregate.shape, bf16),
            jax.ShapeDtypeStruct((own + 1, edge, width), bf16),
            jax.ShapeDtypeStruct(halo.shape, bf16),
            jax.ShapeDtypeStruct((near, width // near, width), bf16),
            jax.ShapeDtypeStruct((1, width), f32),
        ),
        in_specs=[smem, vmem, vmem, vmem, hbm, vmem, vmem],
        out_specs=(hbm, vmem, vmem, vmem, vmem),
        scratch_shapes=[
            VMEM(aggregate.shape, bf16),
            VMEM(aggregate.shape, bf16),
            VMEM((own + 1, edge, width), f32),
            VMEM((halo.shape[0] + 1, edge, width), f32),
            VMEM((width, width), f32),
            VMEM((1, width), f32),
            dma((steps,)),
            dma((steps,)),
        ],
        compiler_params=pltpu.CompilerParams(vmem_limit_bytes=24 * MIB + halo.size * 16),
        name="local_pass",
    )(table, aggregate, halo, held, cotangent, weight, bias)


def return_kernel(
    n, scale, table, held, mixed, halo_ref, weight_ref, bias_ref,
    halo_in, pieces_in, bsum_ref, own_grad,
    halo_land, bias_in, near_in, mine, far_in, piece, pieces_land, running, kept,
    halo_s, halo_r, bias_s, bias_r, near_s, near_r, far_s, far_r, piece_s, piece_r,
):
    me = lax.axis_index("dom")
    barrier = greet(n, me)
    near = weight_ref.shape[0]
    far = n // near
    block, seat = lax.div(me, near), lax.rem(me, near)
    number = held.shape[0]
    own = mixed.shape[0] - 1
    turns = (kept.shape[0] - 1) // UNROLL
    early = turns // 3
    pairs = functools.partial(run_pairs, table, 2, number, own, held, mixed, True, running, kept)
    pairs(0, early)
    halo_copy = functools.partial(push, n, me, lambda p: halo_ref.at[p], halo_land, halo_s, halo_r)
    bias_copy = functools.partial(push, n, me, lambda p: bias_ref, bias_in, bias_s, bias_r)

    def inside(src, dst, send_sem, recv_sem, i):
        peer = lax.rem(seat + i, near)
        return pltpu.make_async_remote_copy(
            src_ref=src(peer), dst_ref=dst.at[seat], send_sem=send_sem.at[i],
            recv_sem=recv_sem.at[i], device_id=(block * near + peer,), device_id_type=MESH,
        )

    def across(i):
        peer = lax.rem(block + i, far)
        return pltpu.make_async_remote_copy(
            src_ref=mine, dst_ref=far_in.at[block], send_sem=far_s.at[i],
            recv_sem=far_r.at[i], device_id=(peer * near + seat,), device_id_type=MESH,
        )

    near_copy = functools.partial(inside, lambda p: weight_ref.at[p], near_in, near_s, near_r)
    piece_copy = functools.partial(inside, lambda p: piece, pieces_land, piece_s, piece_r)

    def over(count, step):
        def turn(i, carry):
            step(i)
            return carry

        lax.fori_loop(1, count, turn, 0)

    pl.semaphore_wait(barrier, n - 1)
    over(near, lambda i: near_copy(i).start())
    over(n, lambda i: halo_copy(i).start())
    over(n, lambda i: bias_copy(i).start())
    near_in[seat] = weight_ref[seat]
    bias_in[me] = bias_ref[...]
    halo_land[me] = halo_ref[me]
    pairs(early, turns)
    over(near, lambda i: near_copy(i).wait())
    mine[...] = jnp.sum(near_in[...].astype(f32), axis=0).astype(bf16)
    over(far, lambda i: across(i).start())
    far_in[block] = mine[...]

    def pick(c, carry):
        own_grad[c] = kept[table[3, c]]
        return carry

    lax.fori_loop(0, own, pick, 0)
    over(far, lambda i: across(i).wait())
    piece[...] = (jnp.sum(far_in[...].astype(f32), axis=0) * scale).astype(bf16)
    over(near, lambda i: piece_copy(i).start())
    pieces_land[seat] = piece[...]
    over(n, lambda i: bias_copy(i).wait())
    bsum_ref[...] = jnp.sum(bias_in[...], axis=0) * scale
    over(n, lambda i: halo_copy(i).wait())
    halo_in[...] = halo_land[...]
    over(near, lambda i: piece_copy(i).wait())
    pieces_in[...] = pieces_land[...]


def exchange_return(n, scale, table, held, mixed, halo_grad, weight_part, bias_part):
    vmem = pl.BlockSpec(memory_space=VMEM)
    smem = pl.BlockSpec(memory_space=pltpu.SMEM)
    dma = pltpu.SemaphoreType.DMA
    edge, width = mixed.shape[1:]
    own = mixed.shape[0] - 1
    pairs = pair_slots(held.shape[0], own)
    near = weight_part.shape[0]
    piece = weight_part.shape[1:]
    return pl.pallas_call(
        functools.partial(return_kernel, n, scale),
        out_shape=(
            jax.ShapeDtypeStruct(halo_grad.shape, bf16),
            jax.ShapeDtypeStruct(weight_part.shape, bf16),
            jax.ShapeDtypeStruct(bias_part.shape, f32),
            jax.ShapeDtypeStruct((own, edge, width), bf16),
        ),
        in_specs=[smem] + [vmem] * 5,
        out_specs=(vmem,) * 4,
        scratch_shapes=[
            VMEM(halo_grad.shape, bf16),
            VMEM((n,) + bias_part.shape, f32),
            VMEM(weight_part.shape, bf16),
            VMEM(piece, bf16),
            VMEM((n // near,) + piece, bf16),
            VMEM(piece, bf16),
            VMEM(weight_part.shape, bf16),
            VMEM((edge, width), f32),
            VMEM((pairs + 1, edge, width), bf16),
        ]
        + [dma((n,))] * 4
        + [dma((near,))] * 2
        + [dma((n // near,))] * 2
        + [dma((near,))] * 2,
        compiler_params=pltpu.CompilerParams(
            collective_id=1, has_side_effects=True,
            vmem_limit_bytes=20 * MIB + halo_grad.size * 16,
        ),
        name="return_exchange",
    )(table, held, mixed, halo_grad, weight_part, bias_part)


def final_kernel(
    chosen_ref, returned, pieces, bias_sum, own, out_hbm, wsum_hbm, bsum_hbm,
    out, wsum, bsum, out_sem, small_sem,
):
    rows = own.shape[0]
    step = math.gcd(rows, 512)
    spans = [pl.ds(c * step, step) for c in range(rows // step)]
    wsum[...] = pieces[...].astype(f32)
    bsum[...] = bias_sum[...]
    outs = [
        pltpu.make_async_copy(wsum, wsum_hbm, small_sem.at[0]),
        pltpu.make_async_copy(bsum, bsum_hbm, small_sem.at[1]),
    ]
    for copy in outs:
        copy.start()
    slots = chosen_ref.shape[1]
    ids = iota((step, slots), 0)
    for c, span in enumerate(spans):
        hot = jnp.where(ids == chosen_ref[...] - c * step, 1.0, 0.0).astype(bf16)
        collected = jnp.dot(hot, returned[...], preferred_element_type=f32)
        out[span, :] = (own[span, :].astype(f32) + collected).astype(bf16)
        copy = pltpu.make_async_copy(out.at[span], out_hbm.at[span], out_sem.at[c])
        copy.start()
        outs.append(copy)
    for copy in outs:
        copy.wait()


def final_pass(chosen, returned, pieces, bias_sum, own_grad):
    rows, width = own_grad.shape
    vmem = pl.BlockSpec(memory_space=VMEM)
    hbm = pl.BlockSpec(memory_space=pltpu.HBM)
    steps = rows // math.gcd(rows, 512)
    return pl.pallas_call(
        final_kernel,
        out_shape=(
            jax.ShapeDtypeStruct(own_grad.shape, bf16),
            jax.ShapeDtypeStruct(pieces.shape, f32),
            jax.ShapeDtypeStruct(bias_sum.shape, f32),
        ),
        in_specs=[vmem] * 5,
        out_specs=(hbm,) * 3,
        scratch_shapes=[
            VMEM(own_grad.shape, bf16),
            VMEM(pieces.shape, f32),
            VMEM(bias_sum.shape, f32),
            pltpu.SemaphoreType.DMA((steps,)),
            pltpu.SemaphoreType.DMA((2,)),
        ],
        compiler_params=pltpu.CompilerParams(vmem_limit_bytes=12 * MIB + returned.size * 32),
        name="final_pass",
    )(chosen, returned, pieces, bias_sum, own_grad)


def body(
    features, weight, bias_vector, tile_values, tile_row, tile_col, tile_count, send_rows,
    send_count, cotangent,
):
    rows, width = features.shape
    n = lax.axis_size("dom")
    slot_count = send_rows.shape[2]
    edge = tile_values.shape[1]
    slots = n * slot_count
    send_rows = jnp.swapaxes(send_rows, 1, 2).reshape(slot_count, n)
    blocks = lambda a: a.reshape(-1, edge, width)
    halo, chosen, table, held, aggregate = exchange_gather(
        n, send_count, tile_count, send_rows, tile_row, tile_col, blocks(features), tile_values
    )
    activation, mixed, halo_grad, weight_part, bias_part = local_pass(
        math.gcd(n, NEAR), table, aggregate, blocks(halo), held, blocks(cotangent), weight,
        bias_vector.reshape(1, width),
    )
    scale = float(rows * n) ** (-0.5)
    returned, pieces, bias_sum, own_grad = exchange_return(
        n, scale, table, held, mixed, halo_grad.reshape(n, slot_count, width), weight_part,
        bias_part,
    )
    grad_features, weight_sum, bias_sum = final_pass(
        chosen, returned.reshape(slots, width), pieces.reshape(width, width), bias_sum,
        own_grad.reshape(rows, width),
    )
    return (activation.reshape(rows, width), grad_features, weight_sum, bias_sum.reshape(width))


def solution(mesh):
    return jax.shard_map(
        body,
        mesh=mesh,
        in_specs=(
            P("dom", None),
            P(),
            P(),
            P("dom", None, None),
            P("dom", None),
            P("dom", None),
            P("dom"),
            P("dom", None, None),
            P("dom", None),
            P("dom", None),
        ),
        out_specs=(P("dom", None), P("dom", None), P(), P()),
        check_vma=False,
    )
```

```python
import functools
import math

import jax
import jax.numpy as jnp
from jax import lax
from jax.experimental import pallas as pl
from jax.experimental.pallas import tpu as pltpu
from jax.sharding import PartitionSpec as P

MESH = pl.DeviceIdType.MESH
VMEM = pltpu.VMEM
f32 = jnp.float32
bf16 = jnp.bfloat16


def greet(n, me):
    barrier = pltpu.get_barrier_semaphore()

    def signal(i, carry):
        pl.semaphore_signal(
            barrier, inc=1, device_id=(lax.rem(me + i, n),), device_id_type=MESH
        )
        return carry

    lax.fori_loop(1, n, signal, 0)
    return barrier


def push(n, me, src, dst, send_sem, recv_sem, i):
    peer = lax.rem(me + i, n)
    return pltpu.make_async_remote_copy(
        src_ref=src(peer),
        dst_ref=dst.at[me],
        send_sem=send_sem.at[i],
        recv_sem=recv_sem.at[i],
        device_id=(peer,),
        device_id_type=MESH,
    )


LANES = 128
TURNS = 4
NEAR = 8
CHUNK = 16
MIB = 1024 * 1024


def padded(size, step):
    return (size + step - 1) // step * step


def bits(size):
    return max(1, (size - 1).bit_length())


def pair_slots(number, keys):
    return padded((number + keys + 1) // 2, TURNS)


def table_width(number, ext):
    return padded(2 * pair_slots(number, ext), LANES)


def down(row):
    return jnp.broadcast_to(row, (LANES, row.shape[1])).T


def iota(shape, dim):
    return lax.broadcasted_iota(jnp.int32, shape, dim)


def place(position, code, default, width):
    position, code = down(position), down(code - default)
    found = []
    for start in range(0, width, LANES):
        hit = position == iota(position.shape, 1) + start
        found.append(jnp.sum(jnp.where(hit, code, 0), axis=0, keepdims=True) + default)
    return jnp.concatenate(found, axis=1)


def wide_columns(columns, width):
    return jnp.concatenate([columns] * (width // LANES), axis=1)


def rank_of(same, valid):
    number = valid.shape[1]
    before = iota((number, number), 0) < iota((number, number), 1)
    taken = jnp.where(before & same, wide_columns(down(valid), number), 0)
    return jnp.sum(taken, axis=0, keepdims=True)


def pair_table(key, other, valid, zero, slots, width):
    number = key.shape[1]
    key_down, valid_down = down(key), down(valid)
    lane = iota((number, LANES), 1)
    count = jnp.sum(jnp.where(key_down == lane, valid_down, 0), axis=0, keepdims=True)
    pairs = (count + 1) // 2
    pairs_down = down(pairs)
    square = (LANES, LANES)
    upto = iota(square, 0) <= iota(square, 1)
    ends = jnp.sum(jnp.where(upto, pairs_down, 0), axis=0, keepdims=True)
    last = jnp.where(count > 0, ends - 1, slots)
    same = wide_columns(key_down, number) == key
    rank = rank_of(same, valid)
    lower = iota((LANES, number), 0) < key
    base = jnp.sum(jnp.where(lower, wide_columns(pairs_down, number), 0), axis=0, keepdims=True)
    position = jnp.where(valid > 0, 2 * base + rank, -1)
    tile = iota((1, number), 1)
    low, high = bits(number), bits(zero + 1)
    first = jnp.where(rank == 0, 1, 0)
    code = tile + other * (1 << low) + first * (1 << (low + high))
    return place(position, code, zero << low, width), last


def fill_table(table, row, col, count, own, ext):
    number = row.shape[1]
    width = table.shape[1]
    used = iota((1, number), 1) < count
    every = jnp.where(used, 1, 0)
    mine = jnp.where(used & (col < own), 1, 0)
    far = jnp.where(used & (col >= own), 1, 0)
    table[...] = jnp.zeros_like(table)
    order, last = pair_table(row, col, mine, own, pair_slots(number, own), width)
    table[0:1, :] = order
    table[1:2, :LANES] = last
    order, last = pair_table(col, row, every, own, pair_slots(number, ext), width)
    table[2:3, :] = order
    table[3:4, :LANES] = last
    rank = rank_of(iota((number, number), 0) >= 0, far)
    low, high = bits(number), bits(ext)
    code = iota((1, number), 1) + (col + row * (1 << high)) * (1 << low)
    position = jnp.where(far > 0, rank, -1)
    table[4:5, :] = place(position, code, (own + (own << high)) << low, width)
    total = jnp.sum(down(far), axis=0, keepdims=True)
    table[5:6, :LANES] = total


def choose(n, count_ref, rows_ref, wide):
    slots, lanes = rows_ref.shape[0], wide.shape[1]
    slot = iota((slots, 1), 0)
    for p in range(n):
        column = jnp.where(slot < count_ref[0, p], rows_ref[:, p : p + 1], -1)
        wide[pl.ds(p * slots, slots), :] = jnp.broadcast_to(column, (slots, lanes))


def run_pairs(table, line, number, zero, held, source, transposed, running, kept):
    low, high = bits(number), bits(zero + 1)
    slots = kept.shape[0] - 1
    unroll = slots // TURNS
    kept[slots] = jnp.zeros(kept.shape[1:], kept.dtype)
    running[...] = jnp.zeros_like(running)
    axis = 0 if transposed else 1

    def turn(g, carry):
        total = running[...]
        for j in range(unroll):
            p = g * unroll + j
            one, two = table[line, 2 * p], table[line, 2 * p + 1]
            tiles = [held[code & ((1 << low) - 1)] for code in (one, two)]
            blocks = [source[(code >> low) & ((1 << high) - 1)] for code in (one, two)]
            product = lax.dot_general(
                jnp.concatenate(tiles, axis=axis), jnp.concatenate(blocks, axis=0),
                (((axis,), (0,)), ((), ())), preferred_element_type=f32,
            )
            keep = (1 - (one >> (low + high))).astype(f32)
            total = total * keep + product
            kept[p] = total.astype(kept.dtype)
        running[...] = total
        return carry

    lax.fori_loop(0, TURNS, turn, 0)


def gather_kernel(
    n, tile_count, count_hbm, rows_hbm, row_hbm, col_hbm, features_hbm, tiles_hbm,
    halo_ref, chosen_ref, table_ref, held, agg_ref,
    count_ref, rows_ref, row_ref, col_ref,
    source, wide, total, sent, landed, table, running, kept,
    send_sem, recv_sem, load_sem, tile_sem, table_sem, small_sem,
):
    me = lax.axis_index("dom")
    own = features_hbm.shape[0]
    edge, width = features_hbm.shape[1:]
    number = tiles_hbm.shape[0]
    step = math.gcd(own, 4)
    smalls = [
        pltpu.make_async_copy(count_hbm, count_ref, small_sem.at[0]),
        pltpu.make_async_copy(rows_hbm, rows_ref, small_sem.at[1]),
        pltpu.make_async_copy(row_hbm, row_ref, small_sem.at[2]),
        pltpu.make_async_copy(col_hbm, col_ref, small_sem.at[3]),
    ]
    for copy in smalls:
        copy.start()
    loads = []
    for c in range(own // step):
        span = pl.ds(c * step, step)
        loads.append(pltpu.make_async_copy(features_hbm.at[span], source.at[span], load_sem.at[c]))
        loads[c].start()
    chunk = math.gcd(number, CHUNK)
    tile_loads = []
    for c in range(number // chunk):
        span = pl.ds(c * chunk, chunk)
        tile_loads.append(pltpu.make_async_copy(tiles_hbm.at[span], held.at[span], tile_sem.at[c]))
    barrier = greet(n, me)
    for copy in smalls:
        copy.wait()
    choose(n, count_ref, rows_ref, wide)
    lane = iota(wide.shape, 1)
    for c in range(own // step):
        hot = jnp.concatenate(
            [
                jnp.where(wide[...] == lane + (c * step * edge + j), 1.0, 0.0).astype(bf16)
                for j in range(0, step * edge, LANES)
            ],
            axis=1,
        )
        loads[c].wait()
        if c == own // step - 1:
            for load in tile_loads:
                load.start()
        block = source[pl.ds(c * step, step)].reshape(step * edge, width)
        part = jnp.dot(hot, block, preferred_element_type=f32)
        if c == 0:
            total[...] = part
        else:
            total[...] += part
    sent[...] = total[...].astype(bf16).reshape(sent.shape)
    pl.semaphore_wait(barrier, n - 1)
    copy = functools.partial(push, n, me, lambda p: sent.at[p], landed, send_sem, recv_sem)

    def start(i, carry):
        copy(i).start()
        return carry

    def finish(i, carry):
        copy(i).wait()
        return carry

    lax.fori_loop(1, n, start, 0)
    landed[me] = sent[me]
    ext = own + wide.shape[0] // edge
    fill_table(table_ref, row_ref[...], col_ref[...], tile_count[0], own, ext)
    move = pltpu.make_async_copy(table_ref, table, table_sem)
    move.start()
    chosen_ref[...] = wide[...].T[:1, :]
    source[own] = jnp.zeros((edge, width), bf16)
    for load in tile_loads:
        load.wait()
    move.wait()
    run_pairs(table, 0, number, own, held, source, False, running, kept)

    def pick(r, carry):
        agg_ref[r] = kept[table[1, r]]
        return carry

    lax.fori_loop(0, own, pick, 0)
    lax.fori_loop(1, n, finish, 0)
    halo_ref[...] = landed[...]


def exchange_gather(n, send_count, tile_count, send_rows, tile_row, tile_col, features, tiles):
    own, edge, width = features.shape
    number = tiles.shape[0]
    slot_count = send_rows.shape[0]
    slots = n * slot_count
    block = (n, slot_count, width)
    pairs = pair_slots(number, own)
    table = (8, table_width(number, own + slots // edge))
    vmem = pl.BlockSpec(memory_space=VMEM)
    smem = pl.BlockSpec(memory_space=pltpu.SMEM)
    hbm = pl.BlockSpec(memory_space=pltpu.HBM)
    dma = pltpu.SemaphoreType.DMA
    return pl.pallas_call(
        functools.partial(gather_kernel, n),
        out_shape=(
            jax.ShapeDtypeStruct(block, bf16),
            jax.ShapeDtypeStruct((1, slots), jnp.int32),
            jax.ShapeDtypeStruct(table, jnp.int32),
            jax.ShapeDtypeStruct(tiles.shape, bf16),
            jax.ShapeDtypeStruct(features.shape, bf16),
        ),
        in_specs=[smem] + [hbm] * 6,
        out_specs=(vmem,) * 5,
        scratch_shapes=[
            pltpu.SMEM(send_count.shape, jnp.int32),
            VMEM(send_rows.shape, jnp.int32),
            VMEM(tile_row.shape, jnp.int32),
            VMEM(tile_col.shape, jnp.int32),
            VMEM((own + 1, edge, width), bf16),
            VMEM((slots, LANES), jnp.int32),
            VMEM((slots, width), f32),
            VMEM(block, bf16),
            VMEM(block, bf16),
            pltpu.SMEM(table, jnp.int32),
            VMEM((edge, width), f32),
            VMEM((pairs + 1, edge, width), bf16),
            dma((n,)),
            dma((n,)),
            dma((own // math.gcd(own, 4),)),
            dma((number // math.gcd(number, CHUNK),)),
            dma,
            dma((4,)),
        ],
        compiler_params=pltpu.CompilerParams(
            collective_id=0, has_side_effects=True, vmem_limit_bytes=24 * MIB + slots * 8192
        ),
        name="gather_exchange",
    )(
        tile_count,
        *[
            pltpu.with_memory_space_constraint(a, pltpu.HBM)
            for a in (send_count, send_rows, tile_row, tile_col, features, tiles)
        ],
    )


GROUP = 4


def boundary_kernel(table, halo, held, extra):
    own = extra.shape[0] - 1
    low, high = bits(held.shape[0]), bits(own + halo.shape[0])

    @pl.loop(0, own + 1)
    def _(r):
        extra[r] = jnp.zeros(extra.shape[1:], f32)

    @pl.loop(0, (table[5, 0] + GROUP - 1) // GROUP)
    def _(g):
        for j in range(GROUP):
            code = table[4, g * GROUP + j]
            col = ((code >> low) & ((1 << high) - 1)) - own
            extra[code >> (low + high)] += jnp.dot(
                held[code & ((1 << low) - 1)], halo[col], preferred_element_type=f32
            )


def boundary_pass(own, table, halo, held):
    edge, width = halo.shape[1:]
    vmem = pl.BlockSpec(memory_space=VMEM)
    return pl.pallas_call(
        boundary_kernel,
        out_shape=jax.ShapeDtypeStruct((own + 1, edge, width), f32),
        in_specs=[pl.BlockSpec(memory_space=pltpu.SMEM), vmem, vmem],
        out_specs=vmem,
        compiler_params=pltpu.CompilerParams(vmem_limit_bytes=4 * MIB),
        name="boundary_pass",
    )(table, halo, held)


def return_kernel(
    n, near, slot_count, scale,
    table_ref, held, aggregate, extra, cot, weight, bias,
    halo_in, pieces_in, bsum_ref, own_grad, act,
    table, mixed, wsum, bsum, halo_ref, halo_land, weight_ref, near_in, mine, far_in, piece,
    pieces_land, bias_ref, bias_near, bias_mine, bias_far, running, kept,
    halo_s, halo_r, near_s, near_r, far_s, far_r, piece_s, piece_r,
    bias_near_s, bias_near_r, bias_far_s, bias_far_r, table_sem,
):
    me = lax.axis_index("dom")
    move = pltpu.make_async_copy(table_ref, table, table_sem)
    move.start()
    barrier = greet(n, me)
    far = n // near
    block, seat = lax.div(me, near), lax.rem(me, near)
    number = held.shape[0]
    own, edge, width = aggregate.shape
    step = math.gcd(own, 4)
    wsum[...] = jnp.zeros_like(wsum)
    bsum[...] = jnp.zeros_like(bsum)

    def activate(b, carry):
        span = pl.ds(b * step, step)
        agg = (aggregate[span].astype(f32) + extra[span]).astype(bf16).reshape(step * edge, width)
        linear = jnp.dot(agg, weight[...], preferred_element_type=f32) + bias[...]
        sig = 0.5 * jnp.tanh(0.5 * linear) + 0.5
        value = linear * sig
        act[span] = value.astype(bf16).reshape(step, edge, width)
        slope = sig + value * (1.0 - sig)
        grad = (cot[span].reshape(step * edge, width).astype(f32) * slope).astype(bf16)
        wsum[...] += lax.dot_general(
            agg, grad, (((0,), (0,)), ((), ())), preferred_element_type=f32
        )
        bsum[...] += jnp.sum(grad.astype(f32), axis=0, keepdims=True)
        back = lax.dot_general(
            grad, weight[...], (((1,), (1,)), ((), ())), preferred_element_type=f32
        )
        mixed[span] = back.astype(bf16).reshape(step, edge, width)
        return carry

    lax.fori_loop(0, own // step, activate, 0, unroll=True)
    mixed[own] = jnp.zeros((edge, width), bf16)
    weight_ref[...] = wsum[...].astype(bf16).reshape(weight_ref.shape)
    bias_ref[...] = bsum[...]
    halo_copy = functools.partial(push, n, me, lambda p: halo_ref.at[p], halo_land, halo_s, halo_r)

    def inside(src, dst, send_sem, recv_sem, i):
        peer = lax.rem(seat + i, near)
        return pltpu.make_async_remote_copy(
            src_ref=src(peer), dst_ref=dst.at[seat], send_sem=send_sem.at[i],
            recv_sem=recv_sem.at[i], device_id=(block * near + peer,), device_id_type=MESH,
        )

    def across(src, dst, send_sem, recv_sem, i):
        peer = lax.rem(block + i, far)
        return pltpu.make_async_remote_copy(
            src_ref=src, dst_ref=dst.at[block], send_sem=send_sem.at[i],
            recv_sem=recv_sem.at[i], device_id=(peer * near + seat,), device_id_type=MESH,
        )

    near_copy = functools.partial(inside, lambda p: weight_ref.at[p], near_in, near_s, near_r)
    piece_copy = functools.partial(inside, lambda p: piece, pieces_land, piece_s, piece_r)
    bias_one = functools.partial(inside, lambda p: bias_ref, bias_near, bias_near_s, bias_near_r)
    far_copy = functools.partial(across, mine, far_in, far_s, far_r)
    bias_two = functools.partial(across, bias_mine, bias_far, bias_far_s, bias_far_r)

    def over(count, step):
        def turn(i, carry):
            step(i)
            return carry

        lax.fori_loop(1, count, turn, 0)

    pl.semaphore_wait(barrier, n - 1)
    over(near, lambda i: near_copy(i).start())
    over(near, lambda i: bias_one(i).start())
    near_in[seat] = weight_ref[seat]
    bias_near[seat] = bias_ref[...]
    move.wait()
    run_pairs(table, 2, number, own, held, mixed, True, running, kept)
    each = edge // slot_count

    def load(b, carry):
        halo_ref[pl.ds(b * each, each)] = kept[table[3, own + b]].reshape(each, slot_count, width)
        return carry

    lax.fori_loop(0, n // each, load, 0)
    over(near, lambda i: near_copy(i).wait())
    mine[...] = jnp.sum(near_in[...].astype(f32), axis=0).astype(bf16)
    over(far, lambda i: far_copy(i).start())
    over(n, lambda i: halo_copy(i).start())
    halo_land[me] = halo_ref[me]
    over(near, lambda i: bias_one(i).wait())
    bias_mine[...] = jnp.sum(bias_near[...], axis=0)
    over(far, lambda i: bias_two(i).start())
    far_in[block] = mine[...]
    bias_far[block] = bias_mine[...]

    def pick(c, carry):
        own_grad[c] = kept[table[3, c]]
        return carry

    lax.fori_loop(0, own, pick, 0)
    over(far, lambda i: far_copy(i).wait())
    piece[...] = (jnp.sum(far_in[...].astype(f32), axis=0) * scale).astype(bf16)
    over(near, lambda i: piece_copy(i).start())
    pieces_land[seat] = piece[...]
    over(far, lambda i: bias_two(i).wait())
    bsum_ref[...] = jnp.sum(bias_far[...], axis=0) * scale
    over(n, lambda i: halo_copy(i).wait())
    halo_in[...] = halo_land[...]
    over(near, lambda i: piece_copy(i).wait())
    pieces_in[...] = pieces_land[...]


def exchange_return(
    n, slot_count, scale, table, held, aggregate, extra, cotangent, weight, bias
):
    vmem = pl.BlockSpec(memory_space=VMEM)
    dma = pltpu.SemaphoreType.DMA
    own, edge, width = aggregate.shape
    number = held.shape[0]
    ext = own + n * slot_count // edge
    pairs = pair_slots(number, ext)
    near = math.gcd(n, NEAR)
    far = n // near
    block = (n, slot_count, width)
    piece = (width // near, width)
    return pl.pallas_call(
        functools.partial(return_kernel, n, near, slot_count, scale),
        out_shape=(
            jax.ShapeDtypeStruct(block, bf16),
            jax.ShapeDtypeStruct((near,) + piece, bf16),
            jax.ShapeDtypeStruct((1, width), f32),
            jax.ShapeDtypeStruct((own, edge, width), bf16),
            jax.ShapeDtypeStruct((own, edge, width), bf16),
        ),
        in_specs=[vmem] * 7,
        out_specs=(vmem,) * 5,
        scratch_shapes=[
            pltpu.SMEM(table.shape, jnp.int32),
            VMEM((own + 1, edge, width), bf16),
            VMEM((width, width), f32),
            VMEM((1, width), f32),
            VMEM(block, bf16),
            VMEM(block, bf16),
            VMEM((near,) + piece, bf16),
            VMEM((near,) + piece, bf16),
            VMEM(piece, bf16),
            VMEM((far,) + piece, bf16),
            VMEM(piece, bf16),
            VMEM((near,) + piece, bf16),
            VMEM((1, width), f32),
            VMEM((near, 1, width), f32),
            VMEM((1, width), f32),
            VMEM((far, 1, width), f32),
            VMEM((edge, width), f32),
            VMEM((pairs + 1, edge, width), bf16),
        ]
        + [dma((n,))] * 2
        + [dma((near,))] * 2
        + [dma((far,))] * 2
        + [dma((near,))] * 4
        + [dma((far,))] * 2
        + [dma],
        compiler_params=pltpu.CompilerParams(
            collective_id=1, has_side_effects=True,
            vmem_limit_bytes=20 * MIB + n * slot_count * width * 16,
        ),
        name="return_exchange",
    )(table, held, aggregate, extra, cotangent, weight, bias)


def final_kernel(
    chosen_ref, returned, pieces, bias_sum, own, act, out_hbm, wsum_hbm, bsum_hbm, act_hbm,
    out, wsum, bsum, out_sem, act_sem, small_sem,
):
    rows = own.shape[0]
    step = math.gcd(rows, 512)
    spans = [pl.ds(c * step, step) for c in range(rows // step)]
    wsum[...] = pieces[...].astype(f32)
    bsum[...] = bias_sum[...]
    outs = [
        pltpu.make_async_copy(wsum, wsum_hbm, small_sem.at[0]),
        pltpu.make_async_copy(bsum, bsum_hbm, small_sem.at[1]),
    ]
    outs += [
        pltpu.make_async_copy(act.at[span], act_hbm.at[span], act_sem.at[c])
        for c, span in enumerate(spans)
    ]
    for copy in outs:
        copy.start()
    slots = chosen_ref.shape[1]
    ids = iota((step, slots), 0)
    for c, span in enumerate(spans):
        hot = jnp.where(ids == chosen_ref[...] - c * step, 1.0, 0.0).astype(bf16)
        collected = jnp.dot(hot, returned[...], preferred_element_type=f32)
        out[span, :] = (own[span, :].astype(f32) + collected).astype(bf16)
        copy = pltpu.make_async_copy(out.at[span], out_hbm.at[span], out_sem.at[c])
        copy.start()
        outs.append(copy)
    for copy in outs:
        copy.wait()


def final_pass(chosen, returned, pieces, bias_sum, own_grad, activation):
    rows, width = own_grad.shape
    vmem = pl.BlockSpec(memory_space=VMEM)
    hbm = pl.BlockSpec(memory_space=pltpu.HBM)
    steps = rows // math.gcd(rows, 512)
    return pl.pallas_call(
        final_kernel,
        out_shape=(
            jax.ShapeDtypeStruct(own_grad.shape, bf16),
            jax.ShapeDtypeStruct(pieces.shape, f32),
            jax.ShapeDtypeStruct(bias_sum.shape, f32),
            jax.ShapeDtypeStruct(activation.shape, bf16),
        ),
        in_specs=[vmem] * 6,
        out_specs=(hbm,) * 4,
        scratch_shapes=[
            VMEM(own_grad.shape, bf16),
            VMEM(pieces.shape, f32),
            VMEM(bias_sum.shape, f32),
            pltpu.SemaphoreType.DMA((steps,)),
            pltpu.SemaphoreType.DMA((steps,)),
            pltpu.SemaphoreType.DMA((2,)),
        ],
        compiler_params=pltpu.CompilerParams(vmem_limit_bytes=12 * MIB + returned.size * 32),
        name="final_pass",
    )(chosen, returned, pieces, bias_sum, own_grad, activation)


def body(
    features, weight, bias_vector, tile_values, tile_row, tile_col, tile_count, send_rows,
    send_count, cotangent,
):
    rows, width = features.shape
    n = lax.axis_size("dom")
    slot_count = send_rows.shape[2]
    edge = tile_values.shape[1]
    slots = n * slot_count
    send_rows = jnp.swapaxes(send_rows, 1, 2).reshape(slot_count, n)
    blocks = lambda a: a.reshape(-1, edge, width)
    halo, chosen, table, held, aggregate = exchange_gather(
        n, send_count, tile_count, send_rows, tile_row, tile_col, blocks(features), tile_values
    )
    extra = boundary_pass(rows // edge, table, blocks(halo), held)
    scale = float(rows * n) ** (-0.5)
    returned, pieces, bias_sum, own_grad, activation = exchange_return(
        n, slot_count, scale, table, held, aggregate, extra, blocks(cotangent), weight,
        bias_vector.reshape(1, width),
    )
    grad_features, weight_sum, bias_sum, activation = final_pass(
        chosen, returned.reshape(slots, width), pieces.reshape(width, width), bias_sum,
        own_grad.reshape(rows, width), activation.reshape(rows, width),
    )
    return (activation, grad_features, weight_sum, bias_sum.reshape(width))


def solution(mesh):
    return jax.shard_map(
        body,
        mesh=mesh,
        in_specs=(
            P("dom", None),
            P(),
            P(),
            P("dom", None, None),
            P("dom", None),
            P("dom", None),
            P("dom"),
            P("dom", None, None),
            P("dom", None),
            P("dom", None),
        ),
        out_specs=(P("dom", None), P("dom", None), P(), P()),
        check_vma=False,
    )
```

```python
import functools
import math

import jax
import jax.numpy as jnp
from jax import lax
from jax.experimental import pallas as pl
from jax.experimental.pallas import tpu as pltpu
from jax.sharding import PartitionSpec as P

MESH = pl.DeviceIdType.MESH
VMEM = pltpu.VMEM
f32 = jnp.float32
bf16 = jnp.bfloat16


def greet(n, me):
    barrier = pltpu.get_barrier_semaphore()

    def signal(i, carry):
        pl.semaphore_signal(
            barrier, inc=1, device_id=(lax.rem(me + i, n),), device_id_type=MESH
        )
        return carry

    lax.fori_loop(1, n, signal, 0)
    return barrier


def push(n, me, src, dst, send_sem, recv_sem, i):
    peer = lax.rem(me + i, n)
    return pltpu.make_async_remote_copy(
        src_ref=src(peer),
        dst_ref=dst.at[me],
        send_sem=send_sem.at[i],
        recv_sem=recv_sem.at[i],
        device_id=(peer,),
        device_id_type=MESH,
    )


LANES = 128
TURNS = 2
NEAR = 8
CHUNK = 16
MIB = 1024 * 1024


def padded(size, step):
    return (size + step - 1) // step * step


def bits(size):
    return max(1, (size - 1).bit_length())


def pair_slots(number, keys):
    return padded((number + keys + 1) // 2, TURNS)


def table_width(number, ext):
    return padded(2 * pair_slots(number, ext), LANES)


def down(row):
    return jnp.broadcast_to(row, (LANES, row.shape[1])).T


def iota(shape, dim):
    return lax.broadcasted_iota(jnp.int32, shape, dim)


def place(position, code, default, width):
    position, code = down(position), down(code - default)
    found = []
    for start in range(0, width, LANES):
        hit = position == iota(position.shape, 1) + start
        found.append(jnp.sum(jnp.where(hit, code, 0), axis=0, keepdims=True) + default)
    return jnp.concatenate(found, axis=1)


def wide_columns(columns, width):
    return jnp.concatenate([columns] * (width // LANES), axis=1)


def rank_of(same, valid):
    number = valid.shape[1]
    before = iota((number, number), 0) < iota((number, number), 1)
    taken = jnp.where(before & same, wide_columns(down(valid), number), 0)
    return jnp.sum(taken, axis=0, keepdims=True)


def pair_table(key, other, valid, zero, slots, width):
    number = key.shape[1]
    key_down, valid_down = down(key), down(valid)
    lane = iota((number, LANES), 1)
    count = jnp.sum(jnp.where(key_down == lane, valid_down, 0), axis=0, keepdims=True)
    pairs = (count + 1) // 2
    pairs_down = down(pairs)
    square = (LANES, LANES)
    upto = iota(square, 0) <= iota(square, 1)
    ends = jnp.sum(jnp.where(upto, pairs_down, 0), axis=0, keepdims=True)
    last = jnp.where(count > 0, ends - 1, slots)
    same = wide_columns(key_down, number) == key
    rank = rank_of(same, valid)
    lower = iota((LANES, number), 0) < key
    base = jnp.sum(jnp.where(lower, wide_columns(pairs_down, number), 0), axis=0, keepdims=True)
    position = jnp.where(valid > 0, 2 * base + rank, -1)
    tile = iota((1, number), 1)
    low, high = bits(number), bits(zero + 1)
    first = jnp.where(rank == 0, 1, 0)
    code = tile + other * (1 << low) + first * (1 << (low + high))
    return place(position, code, zero << low, width), last


def fill_table(table, row, col, count, own, ext):
    number = row.shape[1]
    width = table.shape[1]
    used = iota((1, number), 1) < count
    every = jnp.where(used, 1, 0)
    mine = jnp.where(used & (col < own), 1, 0)
    far = jnp.where(used & (col >= own), 1, 0)
    table[...] = jnp.zeros_like(table)
    order, last = pair_table(row, col, mine, own, pair_slots(number, own), width)
    table[0:1, :] = order
    table[1:2, :LANES] = last
    order, last = pair_table(col, row, every, own, pair_slots(number, ext), width)
    table[2:3, :] = order
    table[3:4, :LANES] = last
    rank = rank_of(iota((number, number), 0) >= 0, far)
    low, high = bits(number), bits(ext)
    code = iota((1, number), 1) + (col + row * (1 << high)) * (1 << low)
    position = jnp.where(far > 0, rank, -1)
    table[4:5, :] = place(position, code, (own + (own << high)) << low, width)
    total = jnp.sum(down(far), axis=0, keepdims=True)
    table[5:6, :LANES] = total


def choose(n, count_ref, rows_ref, wide):
    slots, lanes = rows_ref.shape[0], wide.shape[1]
    slot = iota((slots, 1), 0)
    for p in range(n):
        column = jnp.where(slot < count_ref[0, p], rows_ref[:, p : p + 1], -1)
        wide[pl.ds(p * slots, slots), :] = jnp.broadcast_to(column, (slots, lanes))


def run_pairs(table, line, number, zero, held, source, transposed, running, kept):
    low, high = bits(number), bits(zero + 1)
    slots = kept.shape[0] - 1
    unroll = slots // TURNS
    kept[slots] = jnp.zeros(kept.shape[1:], kept.dtype)
    running[...] = jnp.zeros_like(running)
    axis = 0 if transposed else 1

    def turn(g, carry):
        total = running[...]
        for j in range(unroll):
            p = g * unroll + j
            one, two = table[line, 2 * p], table[line, 2 * p + 1]
            tiles = [held[code & ((1 << low) - 1)] for code in (one, two)]
            blocks = [source[(code >> low) & ((1 << high) - 1)] for code in (one, two)]
            product = lax.dot_general(
                jnp.concatenate(tiles, axis=axis), jnp.concatenate(blocks, axis=0),
                (((axis,), (0,)), ((), ())), preferred_element_type=f32,
            )
            keep = (1 - (one >> (low + high))).astype(f32)
            total = total * keep + product
            kept[p] = total.astype(kept.dtype)
        running[...] = total
        return carry

    lax.fori_loop(0, TURNS, turn, 0)


def gather_kernel(
    n, tile_count, count_hbm, rows_hbm, row_hbm, col_hbm, features_hbm, tiles_hbm,
    halo_ref, chosen_ref, table_ref, held, agg_ref,
    count_ref, rows_ref, row_ref, col_ref,
    source, wide, total, sent, landed, table, running, kept,
    send_sem, recv_sem, load_sem, tile_sem, table_sem, small_sem,
):
    me = lax.axis_index("dom")
    own = features_hbm.shape[0]
    edge, width = features_hbm.shape[1:]
    number = tiles_hbm.shape[0]
    step = math.gcd(own, 4)
    smalls = [
        pltpu.make_async_copy(count_hbm, count_ref, small_sem.at[0]),
        pltpu.make_async_copy(rows_hbm, rows_ref, small_sem.at[1]),
        pltpu.make_async_copy(row_hbm, row_ref, small_sem.at[2]),
        pltpu.make_async_copy(col_hbm, col_ref, small_sem.at[3]),
    ]
    for copy in smalls:
        copy.start()
    loads = []
    for c in range(own // step):
        span = pl.ds(c * step, step)
        loads.append(pltpu.make_async_copy(features_hbm.at[span], source.at[span], load_sem.at[c]))
        loads[c].start()
    chunk = math.gcd(number, CHUNK)
    tile_loads = []
    for c in range(number // chunk):
        span = pl.ds(c * chunk, chunk)
        tile_loads.append(pltpu.make_async_copy(tiles_hbm.at[span], held.at[span], tile_sem.at[c]))
    barrier = greet(n, me)
    for copy in smalls:
        copy.wait()
    choose(n, count_ref, rows_ref, wide)
    lane = iota(wide.shape, 1)
    for c in range(own // step):
        hot = jnp.concatenate(
            [
                jnp.where(wide[...] == lane + (c * step * edge + j), 1.0, 0.0).astype(bf16)
                for j in range(0, step * edge, LANES)
            ],
            axis=1,
        )
        loads[c].wait()
        if c == own // step - 1:
            for load in tile_loads:
                load.start()
        block = source[pl.ds(c * step, step)].reshape(step * edge, width)
        part = jnp.dot(hot, block, preferred_element_type=f32)
        if c == 0:
            total[...] = part
        else:
            total[...] += part
    sent[...] = total[...].astype(bf16).reshape(sent.shape)
    pl.semaphore_wait(barrier, n - 1)
    copy = functools.partial(push, n, me, lambda p: sent.at[p], landed, send_sem, recv_sem)

    def start(i, carry):
        copy(i).start()
        return carry

    def finish(i, carry):
        copy(i).wait()
        return carry

    lax.fori_loop(1, n, start, 0)
    landed[me] = sent[me]
    ext = own + wide.shape[0] // edge
    fill_table(table_ref, row_ref[...], col_ref[...], tile_count[0], own, ext)
    move = pltpu.make_async_copy(table_ref, table, table_sem)
    move.start()
    chosen_ref[...] = wide[...].T[:1, :]
    source[own] = jnp.zeros((edge, width), bf16)
    for load in tile_loads:
        load.wait()
    move.wait()
    run_pairs(table, 0, number, own, held, source, False, running, kept)

    def pick(r, carry):
        agg_ref[r] = kept[table[1, r]]
        return carry

    lax.fori_loop(0, own, pick, 0)
    lax.fori_loop(1, n, finish, 0)
    halo_ref[...] = landed[...]


def exchange_gather(n, send_count, tile_count, send_rows, tile_row, tile_col, features, tiles):
    own, edge, width = features.shape
    number = tiles.shape[0]
    slot_count = send_rows.shape[0]
    slots = n * slot_count
    block = (n, slot_count, width)
    pairs = pair_slots(number, own)
    table = (8, table_width(number, own + slots // edge))
    vmem = pl.BlockSpec(memory_space=VMEM)
    smem = pl.BlockSpec(memory_space=pltpu.SMEM)
    hbm = pl.BlockSpec(memory_space=pltpu.HBM)
    dma = pltpu.SemaphoreType.DMA
    return pl.pallas_call(
        functools.partial(gather_kernel, n),
        out_shape=(
            jax.ShapeDtypeStruct(block, bf16),
            jax.ShapeDtypeStruct((1, slots), jnp.int32),
            jax.ShapeDtypeStruct(table, jnp.int32),
            jax.ShapeDtypeStruct(tiles.shape, bf16),
            jax.ShapeDtypeStruct(features.shape, bf16),
        ),
        in_specs=[smem] + [hbm] * 6,
        out_specs=(vmem,) * 5,
        scratch_shapes=[
            pltpu.SMEM(send_count.shape, jnp.int32),
            VMEM(send_rows.shape, jnp.int32),
            VMEM(tile_row.shape, jnp.int32),
            VMEM(tile_col.shape, jnp.int32),
            VMEM((own + 1, edge, width), bf16),
            VMEM((slots, LANES), jnp.int32),
            VMEM((slots, width), f32),
            VMEM(block, bf16),
            VMEM(block, bf16),
            pltpu.SMEM(table, jnp.int32),
            VMEM((edge, width), f32),
            VMEM((pairs + 1, edge, width), bf16),
            dma((n,)),
            dma((n,)),
            dma((own // math.gcd(own, 4),)),
            dma((number // math.gcd(number, CHUNK),)),
            dma,
            dma((4,)),
        ],
        compiler_params=pltpu.CompilerParams(
            collective_id=0, has_side_effects=True, vmem_limit_bytes=24 * MIB + slots * 8192
        ),
        name="gather_exchange",
    )(
        tile_count,
        *[
            pltpu.with_memory_space_constraint(a, pltpu.HBM)
            for a in (send_count, send_rows, tile_row, tile_col, features, tiles)
        ],
    )


GROUP = 16


def boundary_kernel(table, halo, held, extra):
    own = extra.shape[0] - 1
    low, high = bits(held.shape[0]), bits(own + halo.shape[0])

    @pl.loop(0, own + 1)
    def _(r):
        extra[r] = jnp.zeros(extra.shape[1:], f32)

    @pl.loop(0, (table[5, 0] + GROUP - 1) // GROUP)
    def _(g):
        for j in range(GROUP):
            code = table[4, g * GROUP + j]
            col = ((code >> low) & ((1 << high) - 1)) - own
            extra[code >> (low + high)] += jnp.dot(
                held[code & ((1 << low) - 1)], halo[col], preferred_element_type=f32
            )


def boundary_pass(own, table, halo, held):
    edge, width = halo.shape[1:]
    vmem = pl.BlockSpec(memory_space=VMEM)
    return pl.pallas_call(
        boundary_kernel,
        out_shape=jax.ShapeDtypeStruct((own + 1, edge, width), f32),
        in_specs=[pl.BlockSpec(memory_space=pltpu.SMEM), vmem, vmem],
        out_specs=vmem,
        compiler_params=pltpu.CompilerParams(vmem_limit_bytes=4 * MIB),
        name="boundary_pass",
    )(table, halo, held)


SPLIT = 8


def split(total):
    upper = total.astype(bf16).astype(f32)
    row = iota((SPLIT, total.shape[1]), 0)
    return jnp.where(row == 0, upper, jnp.where(row == 1, total - upper, 0.0)).astype(bf16)


def return_kernel(
    n, near, slot_count, scale,
    table_ref, held, aggregate, extra, cot, weight, bias,
    halo_in, pieces_in, bsum_ref, own_grad, act,
    table, mixed, wsum, bsum, halo_ref, halo_land, weight_ref, near_in, mine, far_in, piece,
    pieces_land, running, kept,
    halo_s, halo_r, near_s, near_r, far_s, far_r, piece_s, piece_r, table_sem,
):
    me = lax.axis_index("dom")
    move = pltpu.make_async_copy(table_ref, table, table_sem)
    move.start()
    barrier = greet(n, me)
    far = n // near
    block, seat = lax.div(me, near), lax.rem(me, near)
    number = held.shape[0]
    own, edge, width = aggregate.shape
    step = math.gcd(own, 4)
    wsum[...] = jnp.zeros_like(wsum)
    bsum[...] = jnp.zeros_like(bsum)

    def activate(b, carry):
        span = pl.ds(b * step, step)
        agg = (aggregate[span].astype(f32) + extra[span]).astype(bf16).reshape(step * edge, width)
        linear = jnp.dot(agg, weight[...], preferred_element_type=f32) + bias[...]
        sig = 0.5 * jnp.tanh(0.5 * linear) + 0.5
        value = linear * sig
        act[span] = value.astype(bf16).reshape(step, edge, width)
        slope = sig + value * (1.0 - sig)
        grad = (cot[span].reshape(step * edge, width).astype(f32) * slope).astype(bf16)
        wsum[...] += lax.dot_general(
            agg, grad, (((0,), (0,)), ((), ())), preferred_element_type=f32
        )
        bsum[...] += jnp.sum(grad.astype(f32), axis=0, keepdims=True)
        back = lax.dot_general(
            grad, weight[...], (((1,), (1,)), ((), ())), preferred_element_type=f32
        )
        mixed[span] = back.astype(bf16).reshape(step, edge, width)
        return carry

    lax.fori_loop(0, own // step, activate, 0, unroll=True)
    mixed[own] = jnp.zeros((edge, width), bf16)
    rows = piece.shape[0]
    weight_ref[:, :rows, :] = wsum[...].astype(bf16).reshape(near, rows, width)
    weight_ref[:, rows:, :] = jnp.broadcast_to(split(bsum[...])[None], (near, SPLIT, width))
    halo_copy = functools.partial(push, n, me, lambda p: halo_ref.at[p], halo_land, halo_s, halo_r)

    def inside(src, dst, send_sem, recv_sem, i):
        peer = lax.rem(seat + i, near)
        return pltpu.make_async_remote_copy(
            src_ref=src(peer), dst_ref=dst.at[seat], send_sem=send_sem.at[i],
            recv_sem=recv_sem.at[i], device_id=(block * near + peer,), device_id_type=MESH,
        )

    def across(src, dst, send_sem, recv_sem, i):
        peer = lax.rem(block + i, far)
        return pltpu.make_async_remote_copy(
            src_ref=src, dst_ref=dst.at[block], send_sem=send_sem.at[i],
            recv_sem=recv_sem.at[i], device_id=(peer * near + seat,), device_id_type=MESH,
        )

    near_copy = functools.partial(inside, lambda p: weight_ref.at[p], near_in, near_s, near_r)
    piece_copy = functools.partial(inside, lambda p: piece, pieces_land, piece_s, piece_r)
    far_copy = functools.partial(across, mine, far_in, far_s, far_r)

    def over(count, step):
        def turn(i, carry):
            step(i)
            return carry

        lax.fori_loop(1, count, turn, 0)

    pl.semaphore_wait(barrier, n - 1)
    over(near, lambda i: near_copy(i).start())
    near_in[seat] = weight_ref[seat]
    move.wait()
    run_pairs(table, 2, number, own, held, mixed, True, running, kept)
    each = edge // slot_count

    def load(b, carry):
        halo_ref[pl.ds(b * each, each)] = kept[table[3, own + b]].reshape(each, slot_count, width)
        return carry

    lax.fori_loop(0, n // each, load, 0)
    over(near, lambda i: near_copy(i).wait())
    summed = jnp.sum(near_in[...].astype(f32), axis=0)
    mine[:rows, :] = summed[:rows].astype(bf16)
    mine[rows:, :] = split(summed[rows : rows + 1] + summed[rows + 1 : rows + 2])
    over(far, lambda i: far_copy(i).start())
    over(n, lambda i: halo_copy(i).start())
    halo_land[me] = halo_ref[me]
    far_in[block] = mine[...]

    def pick(c, carry):
        own_grad[c] = kept[table[3, c]]
        return carry

    lax.fori_loop(0, own, pick, 0)
    over(far, lambda i: far_copy(i).wait())
    summed = jnp.sum(far_in[...].astype(f32), axis=0) * scale
    piece[...] = summed[:rows].astype(bf16)
    over(near, lambda i: piece_copy(i).start())
    pieces_land[seat] = piece[...]
    bsum_ref[...] = summed[rows : rows + 1] + summed[rows + 1 : rows + 2]
    over(n, lambda i: halo_copy(i).wait())
    halo_in[...] = halo_land[...]
    over(near, lambda i: piece_copy(i).wait())
    pieces_in[...] = pieces_land[...]


def exchange_return(
    n, slot_count, scale, table, held, aggregate, extra, cotangent, weight, bias
):
    vmem = pl.BlockSpec(memory_space=VMEM)
    dma = pltpu.SemaphoreType.DMA
    own, edge, width = aggregate.shape
    number = held.shape[0]
    ext = own + n * slot_count // edge
    pairs = pair_slots(number, ext)
    near = math.gcd(n, NEAR)
    far = n // near
    block = (n, slot_count, width)
    piece = (width // near, width)
    longer = (piece[0] + SPLIT, width)
    return pl.pallas_call(
        functools.partial(return_kernel, n, near, slot_count, scale),
        out_shape=(
            jax.ShapeDtypeStruct(block, bf16),
            jax.ShapeDtypeStruct((near,) + piece, bf16),
            jax.ShapeDtypeStruct((1, width), f32),
            jax.ShapeDtypeStruct((own, edge, width), bf16),
            jax.ShapeDtypeStruct((own, edge, width), bf16),
        ),
        in_specs=[vmem] * 7,
        out_specs=(vmem,) * 5,
        scratch_shapes=[
            pltpu.SMEM(table.shape, jnp.int32),
            VMEM((own + 1, edge, width), bf16),
            VMEM((width, width), f32),
            VMEM((1, width), f32),
            VMEM(block, bf16),
            VMEM(block, bf16),
            VMEM((near,) + longer, bf16),
            VMEM((near,) + longer, bf16),
            VMEM(longer, bf16),
            VMEM((far,) + longer, bf16),
            VMEM(piece, bf16),
            VMEM((near,) + piece, bf16),
            VMEM((edge, width), f32),
            VMEM((pairs + 1, edge, width), bf16),
        ]
        + [dma((n,))] * 2
        + [dma((near,))] * 2
        + [dma((far,))] * 2
        + [dma((near,))] * 2
        + [dma],
        compiler_params=pltpu.CompilerParams(
            collective_id=1, has_side_effects=True,
            vmem_limit_bytes=20 * MIB + n * slot_count * width * 16,
        ),
        name="return_exchange",
    )(table, held, aggregate, extra, cotangent, weight, bias)


def final_kernel(
    chosen_ref, returned, pieces, bias_sum, own, act, out_hbm, wsum_hbm, bsum_hbm, act_hbm,
    out, wsum, bsum, out_sem, act_sem, small_sem,
):
    rows = own.shape[0]
    step = math.gcd(rows, 512)
    spans = [pl.ds(c * step, step) for c in range(rows // step)]
    wsum[...] = pieces[...].astype(f32)
    bsum[...] = bias_sum[...]
    outs = [
        pltpu.make_async_copy(wsum, wsum_hbm, small_sem.at[0]),
        pltpu.make_async_copy(bsum, bsum_hbm, small_sem.at[1]),
    ]
    outs += [
        pltpu.make_async_copy(act.at[span], act_hbm.at[span], act_sem.at[c])
        for c, span in enumerate(spans)
    ]
    for copy in outs:
        copy.start()
    slots = chosen_ref.shape[1]
    ids = iota((step, slots), 0)
    for c, span in enumerate(spans):
        hot = jnp.where(ids == chosen_ref[...] - c * step, 1.0, 0.0).astype(bf16)
        collected = jnp.dot(hot, returned[...], preferred_element_type=f32)
        out[span, :] = (own[span, :].astype(f32) + collected).astype(bf16)
        copy = pltpu.make_async_copy(out.at[span], out_hbm.at[span], out_sem.at[c])
        copy.start()
        outs.append(copy)
    for copy in outs:
        copy.wait()


def final_pass(chosen, returned, pieces, bias_sum, own_grad, activation):
    rows, width = own_grad.shape
    vmem = pl.BlockSpec(memory_space=VMEM)
    hbm = pl.BlockSpec(memory_space=pltpu.HBM)
    steps = rows // math.gcd(rows, 512)
    return pl.pallas_call(
        final_kernel,
        out_shape=(
            jax.ShapeDtypeStruct(own_grad.shape, bf16),
            jax.ShapeDtypeStruct(pieces.shape, f32),
            jax.ShapeDtypeStruct(bias_sum.shape, f32),
            jax.ShapeDtypeStruct(activation.shape, bf16),
        ),
        in_specs=[vmem] * 6,
        out_specs=(hbm,) * 4,
        scratch_shapes=[
            VMEM(own_grad.shape, bf16),
            VMEM(pieces.shape, f32),
            VMEM(bias_sum.shape, f32),
            pltpu.SemaphoreType.DMA((steps,)),
            pltpu.SemaphoreType.DMA((steps,)),
            pltpu.SemaphoreType.DMA((2,)),
        ],
        compiler_params=pltpu.CompilerParams(vmem_limit_bytes=12 * MIB + returned.size * 32),
        name="final_pass",
    )(chosen, returned, pieces, bias_sum, own_grad, activation)


def body(
    features, weight, bias_vector, tile_values, tile_row, tile_col, tile_count, send_rows,
    send_count, cotangent,
):
    rows, width = features.shape
    n = lax.axis_size("dom")
    slot_count = send_rows.shape[2]
    edge = tile_values.shape[1]
    slots = n * slot_count
    send_rows = jnp.swapaxes(send_rows, 1, 2).reshape(slot_count, n)
    blocks = lambda a: a.reshape(-1, edge, width)
    halo, chosen, table, held, aggregate = exchange_gather(
        n, send_count, tile_count, send_rows, tile_row, tile_col, blocks(features), tile_values
    )
    extra = boundary_pass(rows // edge, table, blocks(halo), held)
    scale = float(rows * n) ** (-0.5)
    returned, pieces, bias_sum, own_grad, activation = exchange_return(
        n, slot_count, scale, table, held, aggregate, extra, blocks(cotangent), weight,
        bias_vector.reshape(1, width),
    )
    grad_features, weight_sum, bias_sum, activation = final_pass(
        chosen, returned.reshape(slots, width), pieces.reshape(width, width), bias_sum,
        own_grad.reshape(rows, width), activation.reshape(rows, width),
    )
    return (activation, grad_features, weight_sum, bias_sum.reshape(width))


def solution(mesh):
    return jax.shard_map(
        body,
        mesh=mesh,
        in_specs=(
            P("dom", None),
            P(),
            P(),
            P("dom", None, None),
            P("dom", None),
            P("dom", None),
            P("dom"),
            P("dom", None, None),
            P("dom", None),
            P("dom", None),
        ),
        out_specs=(P("dom", None), P("dom", None), P(), P()),
        check_vma=False,
    )
```

```python
import functools
import math

import jax
import jax.numpy as jnp
from jax import lax
from jax.experimental import pallas as pl
from jax.experimental.pallas import tpu as pltpu
from jax.sharding import PartitionSpec as P

MESH = pl.DeviceIdType.MESH
VMEM = pltpu.VMEM
f32 = jnp.float32
bf16 = jnp.bfloat16


def greet(n, me):
    barrier = pltpu.get_barrier_semaphore()

    def signal(i, carry):
        pl.semaphore_signal(
            barrier, inc=1, device_id=(lax.rem(me + i, n),), device_id_type=MESH
        )
        return carry

    lax.fori_loop(1, n, signal, 0)
    return barrier


def push(n, me, src, dst, send_sem, recv_sem, i):
    peer = lax.rem(me + i, n)
    return pltpu.make_async_remote_copy(
        src_ref=src(peer),
        dst_ref=dst.at[me],
        send_sem=send_sem.at[i],
        recv_sem=recv_sem.at[i],
        device_id=(peer,),
        device_id_type=MESH,
    )


LANES = 128
TURNS = 2
NEAR = 8
CHUNK = 16
MIB = 1024 * 1024


def padded(size, step):
    return (size + step - 1) // step * step


def bits(size):
    return max(1, (size - 1).bit_length())


def pair_slots(number, keys):
    return padded((number + keys + 1) // 2, TURNS)


def table_width(number, ext):
    return padded(2 * pair_slots(number, ext), LANES)


def down(row):
    return jnp.broadcast_to(row, (LANES, row.shape[1])).T


def iota(shape, dim):
    return lax.broadcasted_iota(jnp.int32, shape, dim)


def place(position, code, default, width):
    position, code = down(position), down(code - default)
    found = []
    for start in range(0, width, LANES):
        hit = position == iota(position.shape, 1) + start
        found.append(jnp.sum(jnp.where(hit, code, 0), axis=0, keepdims=True) + default)
    return jnp.concatenate(found, axis=1)


def wide_columns(columns, width):
    return jnp.concatenate([columns] * (width // LANES), axis=1)


def rank_of(same, valid):
    number = valid.shape[1]
    before = iota((number, number), 0) < iota((number, number), 1)
    taken = jnp.where(before & same, wide_columns(down(valid), number), 0)
    return jnp.sum(taken, axis=0, keepdims=True)


def pair_table(key, other, valid, zero, slots, width):
    number = key.shape[1]
    key_down, valid_down = down(key), down(valid)
    lane = iota((number, LANES), 1)
    count = jnp.sum(jnp.where(key_down == lane, valid_down, 0), axis=0, keepdims=True)
    pairs = (count + 1) // 2
    pairs_down = down(pairs)
    square = (LANES, LANES)
    upto = iota(square, 0) <= iota(square, 1)
    ends = jnp.sum(jnp.where(upto, pairs_down, 0), axis=0, keepdims=True)
    last = jnp.where(count > 0, ends - 1, slots)
    same = wide_columns(key_down, number) == key
    rank = rank_of(same, valid)
    lower = iota((LANES, number), 0) < key
    base = jnp.sum(jnp.where(lower, wide_columns(pairs_down, number), 0), axis=0, keepdims=True)
    position = jnp.where(valid > 0, 2 * base + rank, -1)
    tile = iota((1, number), 1)
    low, high = bits(number), bits(zero + 1)
    first = jnp.where(rank == 0, 1, 0)
    code = tile + other * (1 << low) + first * (1 << (low + high))
    return place(position, code, zero << low, width), last


def fill_table(table, row, col, count, own, ext):
    number = row.shape[1]
    width = table.shape[1]
    used = iota((1, number), 1) < count
    every = jnp.where(used, 1, 0)
    mine = jnp.where(used & (col < own), 1, 0)
    far = jnp.where(used & (col >= own), 1, 0)
    table[...] = jnp.zeros_like(table)
    order, last = pair_table(row, col, mine, own, pair_slots(number, own), width)
    table[0:1, :] = order
    table[1:2, :LANES] = last
    order, last = pair_table(col, row, every, own, pair_slots(number, ext), width)
    table[2:3, :] = order
    table[3:4, :LANES] = last
    rank = rank_of(iota((number, number), 0) >= 0, far)
    low, high = bits(number), bits(ext)
    code = iota((1, number), 1) + (col + row * (1 << high)) * (1 << low)
    position = jnp.where(far > 0, rank, -1)
    table[4:5, :] = place(position, code, (own + (own << high)) << low, width)
    total = jnp.sum(down(far), axis=0, keepdims=True)
    table[5:6, :LANES] = total


def choose(n, count_ref, rows_ref, wide):
    slots, lanes = rows_ref.shape[0], wide.shape[1]
    slot = iota((slots, 1), 0)
    for p in range(n):
        column = jnp.where(slot < count_ref[0, p], rows_ref[:, p : p + 1], -1)
        wide[pl.ds(p * slots, slots), :] = jnp.broadcast_to(column, (slots, lanes))


def run_pairs(table, line, number, zero, held, source, transposed, running, kept):
    low, high = bits(number), bits(zero + 1)
    slots = kept.shape[0] - 1
    unroll = slots // TURNS
    kept[slots] = jnp.zeros(kept.shape[1:], kept.dtype)
    running[...] = jnp.zeros_like(running)
    axis = 0 if transposed else 1

    def turn(g, carry):
        total = running[...]
        for j in range(unroll):
            p = g * unroll + j
            one, two = table[line, 2 * p], table[line, 2 * p + 1]
            tiles = [held[code & ((1 << low) - 1)] for code in (one, two)]
            blocks = [source[(code >> low) & ((1 << high) - 1)] for code in (one, two)]
            product = lax.dot_general(
                jnp.concatenate(tiles, axis=axis), jnp.concatenate(blocks, axis=0),
                (((axis,), (0,)), ((), ())), preferred_element_type=f32,
            )
            keep = (1 - (one >> (low + high))).astype(f32)
            total = total * keep + product
            kept[p] = total.astype(kept.dtype)
        running[...] = total
        return carry

    lax.fori_loop(0, TURNS, turn, 0)


def gather_kernel(
    n, tile_count, count_hbm, rows_hbm, row_hbm, col_hbm, features_hbm, tiles_hbm, cot_hbm,
    halo_ref, chosen_ref, table_ref, held, agg_ref, extra_ref, cot_ref,
    count_ref, rows_ref, row_ref, col_ref,
    source, wide, total, sent, landed, table, running, kept,
    send_sem, recv_sem, load_sem, tile_sem, table_sem, small_sem, cot_sem,
):
    me = lax.axis_index("dom")
    own = features_hbm.shape[0]
    edge, width = features_hbm.shape[1:]
    number = tiles_hbm.shape[0]
    step = math.gcd(own, 4)
    smalls = [
        pltpu.make_async_copy(count_hbm, count_ref, small_sem.at[0]),
        pltpu.make_async_copy(rows_hbm, rows_ref, small_sem.at[1]),
        pltpu.make_async_copy(row_hbm, row_ref, small_sem.at[2]),
        pltpu.make_async_copy(col_hbm, col_ref, small_sem.at[3]),
    ]
    for copy in smalls:
        copy.start()
    loads = []
    for c in range(own // step):
        span = pl.ds(c * step, step)
        loads.append(pltpu.make_async_copy(features_hbm.at[span], source.at[span], load_sem.at[c]))
        loads[c].start()
    chunk = math.gcd(number, CHUNK)
    tile_loads = []
    for c in range(number // chunk):
        span = pl.ds(c * chunk, chunk)
        tile_loads.append(pltpu.make_async_copy(tiles_hbm.at[span], held.at[span], tile_sem.at[c]))
    cot_load = pltpu.make_async_copy(cot_hbm, cot_ref, cot_sem)
    barrier = greet(n, me)
    for copy in smalls:
        copy.wait()
    choose(n, count_ref, rows_ref, wide)
    lane = iota(wide.shape, 1)
    for c in range(own // step):
        hot = jnp.concatenate(
            [
                jnp.where(wide[...] == lane + (c * step * edge + j), 1.0, 0.0).astype(bf16)
                for j in range(0, step * edge, LANES)
            ],
            axis=1,
        )
        loads[c].wait()
        if c == own // step - 1:
            for load in tile_loads:
                load.start()
            cot_load.start()
        block = source[pl.ds(c * step, step)].reshape(step * edge, width)
        part = jnp.dot(hot, block, preferred_element_type=f32)
        if c == 0:
            total[...] = part
        else:
            total[...] += part
    sent[...] = total[...].astype(bf16).reshape(sent.shape)
    pl.semaphore_wait(barrier, n - 1)
    copy = functools.partial(push, n, me, lambda p: sent.at[p], landed, send_sem, recv_sem)

    def start(i, carry):
        copy(i).start()
        return carry

    def finish(i, carry):
        copy(i).wait()
        return carry

    lax.fori_loop(1, n, start, 0)
    landed[me] = sent[me]
    ext = own + wide.shape[0] // edge
    fill_table(table_ref, row_ref[...], col_ref[...], tile_count[0], own, ext)
    move = pltpu.make_async_copy(table_ref, table, table_sem)
    move.start()
    chosen_ref[...] = wide[...].T[:1, :]
    source[own] = jnp.zeros((edge, width), bf16)
    for load in tile_loads:
        load.wait()
    move.wait()
    run_pairs(table, 0, number, own, held, source, False, running, kept)

    def pick(r, carry):
        agg_ref[r] = kept[table[1, r]]
        extra_ref[r] = jnp.zeros(extra_ref.shape[1:], f32)
        return carry

    lax.fori_loop(0, own, pick, 0)
    cot_load.wait()
    lax.fori_loop(1, n, finish, 0)
    halo_ref[...] = landed[...]


def exchange_gather(
    n, send_count, tile_count, send_rows, tile_row, tile_col, features, tiles, cotangent
):
    own, edge, width = features.shape
    number = tiles.shape[0]
    slot_count = send_rows.shape[0]
    slots = n * slot_count
    block = (n, slot_count, width)
    pairs = pair_slots(number, own)
    table = (8, table_width(number, own + slots // edge))
    vmem = pl.BlockSpec(memory_space=VMEM)
    smem = pl.BlockSpec(memory_space=pltpu.SMEM)
    hbm = pl.BlockSpec(memory_space=pltpu.HBM)
    dma = pltpu.SemaphoreType.DMA
    return pl.pallas_call(
        functools.partial(gather_kernel, n),
        out_shape=(
            jax.ShapeDtypeStruct(block, bf16),
            jax.ShapeDtypeStruct((1, slots), jnp.int32),
            jax.ShapeDtypeStruct(table, jnp.int32),
            jax.ShapeDtypeStruct(tiles.shape, bf16),
            jax.ShapeDtypeStruct(features.shape, bf16),
            jax.ShapeDtypeStruct((own + 1, edge, width), f32),
            jax.ShapeDtypeStruct(features.shape, bf16),
        ),
        in_specs=[smem] + [hbm] * 7,
        out_specs=(vmem,) * 7,
        scratch_shapes=[
            pltpu.SMEM(send_count.shape, jnp.int32),
            VMEM(send_rows.shape, jnp.int32),
            VMEM(tile_row.shape, jnp.int32),
            VMEM(tile_col.shape, jnp.int32),
            VMEM((own + 1, edge, width), bf16),
            VMEM((slots, LANES), jnp.int32),
            VMEM((slots, width), f32),
            VMEM(block, bf16),
            VMEM(block, bf16),
            pltpu.SMEM(table, jnp.int32),
            VMEM((edge, width), f32),
            VMEM((pairs + 1, edge, width), bf16),
            dma((n,)),
            dma((n,)),
            dma((own // math.gcd(own, 4),)),
            dma((number // math.gcd(number, CHUNK),)),
            dma,
            dma((4,)),
            dma,
        ],
        compiler_params=pltpu.CompilerParams(
            collective_id=0, has_side_effects=True,
            vmem_limit_bytes=min(60 * MIB, 8 * MIB + slots * 40960),
        ),
        name="gather_exchange",
    )(
        tile_count,
        *[
            pltpu.with_memory_space_constraint(a, pltpu.HBM)
            for a in (send_count, send_rows, tile_row, tile_col, features, tiles, cotangent)
        ],
    )


GROUP = 16


def boundary_kernel(table, halo, held, zeros, extra):
    own = extra.shape[0] - 1
    low, high = bits(held.shape[0]), bits(own + halo.shape[0])

    @pl.loop(0, (table[5, 0] + GROUP - 1) // GROUP)
    def _(g):
        for j in range(GROUP):
            code = table[4, g * GROUP + j]
            col = ((code >> low) & ((1 << high) - 1)) - own
            extra[code >> (low + high)] += jnp.dot(
                held[code & ((1 << low) - 1)], halo[col], preferred_element_type=f32
            )


def boundary_pass(table, halo, held, zeros):
    vmem = pl.BlockSpec(memory_space=VMEM)
    return pl.pallas_call(
        boundary_kernel,
        out_shape=jax.ShapeDtypeStruct(zeros.shape, f32),
        in_specs=[pl.BlockSpec(memory_space=pltpu.SMEM)] + [vmem] * 3,
        out_specs=vmem,
        input_output_aliases={3: 0},
        compiler_params=pltpu.CompilerParams(vmem_limit_bytes=4 * MIB),
        name="boundary_pass",
    )(table, halo, held, zeros)


SPLIT = 8


def split(total):
    upper = total.astype(bf16).astype(f32)
    row = iota((SPLIT, total.shape[1]), 0)
    return jnp.where(row == 0, upper, jnp.where(row == 1, total - upper, 0.0)).astype(bf16)


def return_kernel(
    n, near, slot_count, scale,
    table_ref, held, aggregate, extra, cot, weight, bias,
    halo_in, pieces_in, bsum_ref, own_grad, act,
    table, mixed, wsum, bsum, halo_ref, halo_land, weight_ref, near_in, mine, far_in, piece,
    pieces_land, running, kept,
    halo_s, halo_r, near_s, near_r, far_s, far_r, piece_s, piece_r, table_sem,
):
    me = lax.axis_index("dom")
    move = pltpu.make_async_copy(table_ref, table, table_sem)
    move.start()
    barrier = greet(n, me)
    far = n // near
    block, seat = lax.div(me, near), lax.rem(me, near)
    number = held.shape[0]
    own, edge, width = aggregate.shape
    step = math.gcd(own, 4)
    wsum[...] = jnp.zeros_like(wsum)
    bsum[...] = jnp.zeros_like(bsum)

    def activate(b, carry):
        span = pl.ds(b * step, step)
        agg = (aggregate[span].astype(f32) + extra[span]).astype(bf16).reshape(step * edge, width)
        linear = jnp.dot(agg, weight[...], preferred_element_type=f32) + bias[...]
        sig = 0.5 * jnp.tanh(0.5 * linear) + 0.5
        value = linear * sig
        act[span] = value.astype(bf16).reshape(step, edge, width)
        slope = sig + value * (1.0 - sig)
        grad = (cot[span].reshape(step * edge, width).astype(f32) * slope).astype(bf16)
        wsum[...] += lax.dot_general(
            agg, grad, (((0,), (0,)), ((), ())), preferred_element_type=f32
        )
        bsum[...] += jnp.sum(grad.astype(f32), axis=0, keepdims=True)
        back = lax.dot_general(
            grad, weight[...], (((1,), (1,)), ((), ())), preferred_element_type=f32
        )
        mixed[span] = back.astype(bf16).reshape(step, edge, width)
        return carry

    lax.fori_loop(0, own // step, activate, 0, unroll=True)
    mixed[own] = jnp.zeros((edge, width), bf16)
    rows = piece.shape[0]
    weight_ref[:, :rows, :] = wsum[...].astype(bf16).reshape(near, rows, width)
    weight_ref[:, rows:, :] = jnp.broadcast_to(split(bsum[...])[None], (near, SPLIT, width))
    halo_copy = functools.partial(push, n, me, lambda p: halo_ref.at[p], halo_land, halo_s, halo_r)

    def inside(src, dst, send_sem, recv_sem, i):
        peer = lax.rem(seat + i, near)
        return pltpu.make_async_remote_copy(
            src_ref=src(peer), dst_ref=dst.at[seat], send_sem=send_sem.at[i],
            recv_sem=recv_sem.at[i], device_id=(block * near + peer,), device_id_type=MESH,
        )

    def across(src, dst, send_sem, recv_sem, i):
        peer = lax.rem(block + i, far)
        return pltpu.make_async_remote_copy(
            src_ref=src, dst_ref=dst.at[block], send_sem=send_sem.at[i],
            recv_sem=recv_sem.at[i], device_id=(peer * near + seat,), device_id_type=MESH,
        )

    near_copy = functools.partial(inside, lambda p: weight_ref.at[p], near_in, near_s, near_r)
    piece_copy = functools.partial(inside, lambda p: piece, pieces_land, piece_s, piece_r)
    far_copy = functools.partial(across, mine, far_in, far_s, far_r)

    def over(count, step):
        def turn(i, carry):
            step(i)
            return carry

        lax.fori_loop(1, count, turn, 0)

    pl.semaphore_wait(barrier, n - 1)
    over(near, lambda i: near_copy(i).start())
    near_in[seat] = weight_ref[seat]
    move.wait()
    run_pairs(table, 2, number, own, held, mixed, True, running, kept)
    each = edge // slot_count

    def load(b, carry):
        halo_ref[pl.ds(b * each, each)] = kept[table[3, own + b]].reshape(each, slot_count, width)
        return carry

    lax.fori_loop(0, n // each, load, 0)
    over(near, lambda i: near_copy(i).wait())
    summed = jnp.sum(near_in[...].astype(f32), axis=0)
    mine[:rows, :] = summed[:rows].astype(bf16)
    mine[rows:, :] = split(summed[rows : rows + 1] + summed[rows + 1 : rows + 2])
    over(far, lambda i: far_copy(i).start())
    over(n, lambda i: halo_copy(i).start())
    halo_land[me] = halo_ref[me]
    far_in[block] = mine[...]

    def pick(c, carry):
        own_grad[c] = kept[table[3, c]]
        return carry

    lax.fori_loop(0, own, pick, 0)
    over(far, lambda i: far_copy(i).wait())
    summed = jnp.sum(far_in[...].astype(f32), axis=0) * scale
    piece[...] = summed[:rows].astype(bf16)
    over(near, lambda i: piece_copy(i).start())
    pieces_land[seat] = piece[...]
    bsum_ref[...] = summed[rows : rows + 1] + summed[rows + 1 : rows + 2]
    over(n, lambda i: halo_copy(i).wait())
    halo_in[...] = halo_land[...]
    over(near, lambda i: piece_copy(i).wait())
    pieces_in[...] = pieces_land[...]


def exchange_return(
    n, slot_count, scale, table, held, aggregate, extra, cotangent, weight, bias
):
    vmem = pl.BlockSpec(memory_space=VMEM)
    dma = pltpu.SemaphoreType.DMA
    own, edge, width = aggregate.shape
    number = held.shape[0]
    ext = own + n * slot_count // edge
    pairs = pair_slots(number, ext)
    near = math.gcd(n, NEAR)
    far = n // near
    block = (n, slot_count, width)
    piece = (width // near, width)
    longer = (piece[0] + SPLIT, width)
    return pl.pallas_call(
        functools.partial(return_kernel, n, near, slot_count, scale),
        out_shape=(
            jax.ShapeDtypeStruct(block, bf16),
            jax.ShapeDtypeStruct((near,) + piece, bf16),
            jax.ShapeDtypeStruct((1, width), f32),
            jax.ShapeDtypeStruct((own, edge, width), bf16),
            jax.ShapeDtypeStruct((own, edge, width), bf16),
        ),
        in_specs=[vmem] * 7,
        out_specs=(vmem,) * 5,
        scratch_shapes=[
            pltpu.SMEM(table.shape, jnp.int32),
            VMEM((own + 1, edge, width), bf16),
            VMEM((width, width), f32),
            VMEM((1, width), f32),
            VMEM(block, bf16),
            VMEM(block, bf16),
            VMEM((near,) + longer, bf16),
            VMEM((near,) + longer, bf16),
            VMEM(longer, bf16),
            VMEM((far,) + longer, bf16),
            VMEM(piece, bf16),
            VMEM((near,) + piece, bf16),
            VMEM((edge, width), f32),
            VMEM((pairs + 1, edge, width), bf16),
        ]
        + [dma((n,))] * 2
        + [dma((near,))] * 2
        + [dma((far,))] * 2
        + [dma((near,))] * 2
        + [dma],
        compiler_params=pltpu.CompilerParams(
            collective_id=1, has_side_effects=True,
            vmem_limit_bytes=20 * MIB + n * slot_count * width * 16,
        ),
        name="return_exchange",
    )(table, held, aggregate, extra, cotangent, weight, bias)


def final_step(rows, slots):
    return math.gcd(rows, 1 << max(9, 19 - bits(slots)))


def final_kernel(
    chosen_ref, returned, pieces, bias_sum, own, act, out_hbm, wsum_hbm, bsum_hbm, act_hbm,
    out, wsum, bsum, out_sem, act_sem, small_sem,
):
    rows = own.shape[0]
    step = final_step(rows, chosen_ref.shape[1])
    spans = [pl.ds(c * step, step) for c in range(rows // step)]
    wsum[...] = pieces[...].astype(f32)
    bsum[...] = bias_sum[...]
    outs = [
        pltpu.make_async_copy(wsum, wsum_hbm, small_sem.at[0]),
        pltpu.make_async_copy(bsum, bsum_hbm, small_sem.at[1]),
    ]
    outs += [
        pltpu.make_async_copy(act.at[span], act_hbm.at[span], act_sem.at[c])
        for c, span in enumerate(spans)
    ]
    for copy in outs:
        copy.start()
    slots = chosen_ref.shape[1]
    ids = iota((step, slots), 0)
    for c, span in enumerate(spans):
        hot = jnp.where(ids == chosen_ref[...] - c * step, 1.0, 0.0).astype(bf16)
        collected = jnp.dot(hot, returned[...], preferred_element_type=f32)
        out[span, :] = (own[span, :].astype(f32) + collected).astype(bf16)
        copy = pltpu.make_async_copy(out.at[span], out_hbm.at[span], out_sem.at[c])
        copy.start()
        outs.append(copy)
    for copy in outs:
        copy.wait()


def final_pass(chosen, returned, pieces, bias_sum, own_grad, activation):
    rows, width = own_grad.shape
    vmem = pl.BlockSpec(memory_space=VMEM)
    hbm = pl.BlockSpec(memory_space=pltpu.HBM)
    steps = rows // final_step(rows, returned.shape[0])
    return pl.pallas_call(
        final_kernel,
        out_shape=(
            jax.ShapeDtypeStruct(own_grad.shape, bf16),
            jax.ShapeDtypeStruct(pieces.shape, f32),
            jax.ShapeDtypeStruct(bias_sum.shape, f32),
            jax.ShapeDtypeStruct(activation.shape, bf16),
        ),
        in_specs=[vmem] * 6,
        out_specs=(hbm,) * 4,
        scratch_shapes=[
            VMEM(own_grad.shape, bf16),
            VMEM(pieces.shape, f32),
            VMEM(bias_sum.shape, f32),
            pltpu.SemaphoreType.DMA((steps,)),
            pltpu.SemaphoreType.DMA((steps,)),
            pltpu.SemaphoreType.DMA((2,)),
        ],
        compiler_params=pltpu.CompilerParams(vmem_limit_bytes=12 * MIB + returned.size * 32),
        name="final_pass",
    )(chosen, returned, pieces, bias_sum, own_grad, activation)


def body(
    features, weight, bias_vector, tile_values, tile_row, tile_col, tile_count, send_rows,
    send_count, cotangent,
):
    rows, width = features.shape
    n = lax.axis_size("dom")
    slot_count = send_rows.shape[2]
    edge = tile_values.shape[1]
    slots = n * slot_count
    send_rows = jnp.swapaxes(send_rows, 1, 2).reshape(slot_count, n)
    blocks = lambda a: a.reshape(-1, edge, width)
    halo, chosen, table, held, aggregate, zeros, cotangent = exchange_gather(
        n, send_count, tile_count, send_rows, tile_row, tile_col, blocks(features), tile_values,
        blocks(cotangent),
    )
    extra = boundary_pass(table, blocks(halo), held, zeros)
    scale = float(rows * n) ** (-0.5)
    returned, pieces, bias_sum, own_grad, activation = exchange_return(
        n, slot_count, scale, table, held, aggregate, extra, cotangent, weight,
        bias_vector.reshape(1, width),
    )
    grad_features, weight_sum, bias_sum, activation = final_pass(
        chosen, returned.reshape(slots, width), pieces.reshape(width, width), bias_sum,
        own_grad.reshape(rows, width), activation.reshape(rows, width),
    )
    return (activation, grad_features, weight_sum, bias_sum.reshape(width))


def solution(mesh):
    return jax.shard_map(
        body,
        mesh=mesh,
        in_specs=(
            P("dom", None),
            P(),
            P(),
            P("dom", None, None),
            P("dom", None),
            P("dom", None),
            P("dom"),
            P("dom", None, None),
            P("dom", None),
            P("dom", None),
        ),
        out_specs=(P("dom", None), P("dom", None), P(), P()),
        check_vma=False,
    )
```
